32 devices in a mesh: e: 4 (over z), b: 2 (over y), a: 4 (over x, core).
Axes of the slice: x: 2, y: 2, z: 4, core: 2. Of those that a mesh axis runs over, the one named last changes fastest.
Arguments:
- act_in: bfloat16 [32, 512, 1024], P(('a', 'b'), None, 'e')
- grad_y: bfloat16 [32, 512, 1024], P(('a', 'b'), None, 'e')
- ln1_gain: float32 [1024], P('e')
- ln1_shift: float32 [1024], P('e')
- w_qkv: bfloat16 [3, 1024, 1024], P(None, 'e', ('b', 'a'))
- b_qkv: float32 [3, 16, 64], P(None, 'b')
- w_out: bfloat16 [1024, 1024], P('b', ('e', 'a'))
- b_out: float32 [1024], P('e')
- ln2_gain: float32 [1024], P('e')
- ln2_shift: float32 [1024], P('e')
- w_up: bfloat16 [1024, 4096], P('e', ('b', 'a'))
- b_up: float32 [4096], P('b')
- w_down: bfloat16 [4096, 1024], P('b', ('e', 'a'))
- b_down: float32 [1024], P('e')
Outputs:
- output 1: bfloat16 [32, 512, 1024], P(('a', 'b'), None, 'e')
- output 2: bfloat16 [32, 512, 1024], P(('a', 'b'), None, 'e')
- output 3: float32 [1024], P('e')
- output 4: float32 [1024], P('e')
- output 5: bfloat16 [3, 1024, 1024], P(None, 'e', ('b', 'a'))
- output 6: float32 [3, 16, 64], P(None, 'b')
- output 7: bfloat16 [1024, 1024], P('b', ('e', 'a'))
- output 8: float32 [1024], P('e')
- output 9: float32 [1024], P('e')
- output 10: float32 [1024], P('e')
- output 11: bfloat16 [1024, 4096], P('e', ('b', 'a'))
- output 12: float32 [4096], P('b')
- output 13: bfloat16 [4096, 1024], P('b', ('e', 'a'))
- output 14: float32 [1024], P('e')
All inputs are finite; a program needn't handle non-finite values.
Results may differ from the reference program's by a relative error of at most 0.02.
Values are sent between devices in bfloat16 or wider.
A program may use at most 1 GiB of HBM per device.

```python
import jax
import jax.numpy as jnp
from jax import lax

BATCH_SEQS = 32
SEQ_LEN = 512
HIDDEN = 1024
N_HEADS = 16
HEAD_DIM = 64
FFN_DIM = 4096
LN_EPS = 1e-5


def setup_inputs(seed: int = 0) -> dict:
    sub_keys = jax.random.split(jax.random.key(seed), 16)
    act_shape = (BATCH_SEQS, SEQ_LEN, HIDDEN)
    col_ramp = jnp.linspace(-1.0, 1.0, HIDDEN, dtype=jnp.float32)
    row_amp = jax.random.normal(sub_keys[0], (BATCH_SEQS, SEQ_LEN, 1), jnp.float32)
    x_noise = jax.random.normal(sub_keys[1], act_shape, jnp.float32)
    hid_scale = HIDDEN ** -0.5
    ffn_scale = FFN_DIM ** -0.5
    return {
        'act_in': (x_noise + row_amp * col_ramp).astype(jnp.bfloat16),
        'grad_y': jax.random.normal(sub_keys[2], act_shape, jnp.float32).astype(jnp.bfloat16),
        'ln1_gain': 1.0 + 0.3 * jax.random.normal(sub_keys[3], (HIDDEN,), jnp.float32),
        'ln1_shift': 0.3 * jax.random.normal(sub_keys[4], (HIDDEN,), jnp.float32),
        'w_qkv': (jax.random.normal(sub_keys[5], (3, HIDDEN, HIDDEN), jnp.float32) * hid_scale).astype(jnp.bfloat16),
        'b_qkv': 0.5 * jax.random.normal(sub_keys[6], (3, N_HEADS, HEAD_DIM), jnp.float32),
        'w_out': (jax.random.normal(sub_keys[7], (HIDDEN, HIDDEN), jnp.float32) * hid_scale).astype(jnp.bfloat16),
        'b_out': 0.5 * jax.random.normal(sub_keys[8], (HIDDEN,), jnp.float32),
        'ln2_gain': 1.0 + 0.3 * jax.random.normal(sub_keys[9], (HIDDEN,), jnp.float32),
        'ln2_shift': 0.3 * jax.random.normal(sub_keys[10], (HIDDEN,), jnp.float32),
        'w_up': (jax.random.normal(sub_keys[11], (HIDDEN, FFN_DIM), jnp.float32) * hid_scale).astype(jnp.bfloat16),
        'b_up': 0.5 * jax.random.normal(sub_keys[12], (FFN_DIM,), jnp.float32),
        'w_down': (jax.random.normal(sub_keys[13], (FFN_DIM, HIDDEN), jnp.float32) * ffn_scale).astype(jnp.bfloat16),
        'b_down': 0.5 * jax.random.normal(sub_keys[14], (HIDDEN,), jnp.float32),
    }


def f32_dot(left_op, right_op):
    return jnp.dot(left_op.astype(jnp.float32), right_op.astype(jnp.float32))


def layer_norm(x_wide, ln_gain, ln_shift):
    row_mean = jnp.mean(x_wide, axis=-1, keepdims=True)
    centered = x_wide - row_mean
    variance = jnp.mean(centered * centered, axis=-1, keepdims=True)
    return centered * lax.rsqrt(variance + LN_EPS) * ln_gain + ln_shift


def attend_sequence(qkv_trio):
    q_seq, k_seq, v_seq = qkv_trio
    scores = jnp.einsum('qhd,khd->hqk', q_seq.astype(jnp.float32), k_seq.astype(jnp.float32)) * (HEAD_DIM ** -0.5)
    causal = jnp.arange(SEQ_LEN)[:, None] >= jnp.arange(SEQ_LEN)[None, :]
    scores = jnp.where(causal, scores, -1e30)
    attn_probs = jax.nn.softmax(scores, axis=-1).astype(jnp.bfloat16)
    context = jnp.einsum('hqk,khd->qhd', attn_probs.astype(jnp.float32), v_seq.astype(jnp.float32))
    return context.astype(jnp.bfloat16)


def layer_forward(act_in, ln1_gain, ln1_shift, w_qkv, b_qkv, w_out, b_out, ln2_gain, ln2_shift, w_up, b_up, w_down, b_down):
    n_tokens = BATCH_SEQS * SEQ_LEN
    heads_shape = (BATCH_SEQS, SEQ_LEN, N_HEADS, HEAD_DIM)
    x_rows = act_in.reshape(n_tokens, HIDDEN).astype(jnp.float32)
    h_one = layer_norm(x_rows, ln1_gain, ln1_shift).astype(jnp.bfloat16)
    q_all = (f32_dot(h_one, w_qkv[0]) + b_qkv[0].reshape(HIDDEN)).astype(jnp.bfloat16).reshape(heads_shape)
    k_all = (f32_dot(h_one, w_qkv[1]) + b_qkv[1].reshape(HIDDEN)).astype(jnp.bfloat16).reshape(heads_shape)
    v_all = (f32_dot(h_one, w_qkv[2]) + b_qkv[2].reshape(HIDDEN)).astype(jnp.bfloat16).reshape(heads_shape)
    context = lax.map(jax.checkpoint(attend_sequence), (q_all, k_all, v_all)).reshape(n_tokens, HIDDEN)
    x_one = (x_rows + f32_dot(context, w_out) + b_out).astype(jnp.bfloat16)
    h_two = layer_norm(x_one.astype(jnp.float32), ln2_gain, ln2_shift).astype(jnp.bfloat16)
    mlp_act = jax.nn.gelu(f32_dot(h_two, w_up) + b_up, approximate=True).astype(jnp.bfloat16)
    y_rows = (x_one.astype(jnp.float32) + f32_dot(mlp_act, w_down) + b_down).astype(jnp.bfloat16)
    return y_rows.reshape(BATCH_SEQS, SEQ_LEN, HIDDEN)


def reference(act_in, grad_y, ln1_gain, ln1_shift, w_qkv, b_qkv, w_out, b_out, ln2_gain, ln2_shift, w_up, b_up, w_down, b_down):
    y_out, pullback = jax.vjp(layer_forward, act_in, ln1_gain, ln1_shift, w_qkv, b_qkv, w_out, b_out, ln2_gain, ln2_shift, w_up, b_up, w_down, b_down)
    (grad_x, grad_ln1_gain, grad_ln1_shift, grad_w_qkv, grad_b_qkv, grad_w_out, grad_b_out,
     grad_ln2_gain, grad_ln2_shift, grad_w_up, grad_b_up, grad_w_down, grad_b_down) = pullback(grad_y)
    return (y_out, grad_x, grad_ln1_gain, grad_ln1_shift, grad_w_qkv, grad_b_qkv, grad_w_out, grad_b_out,
            grad_ln2_gain, grad_ln2_shift, grad_w_up, grad_b_up, grad_w_down, grad_b_down)
```

```python
import functools

import jax
import jax.numpy as jnp
from jax import lax
from jax.experimental import pallas as pl
from jax.experimental.pallas import tpu as pltpu
from jax.sharding import Mesh, PartitionSpec as P

LN_EPS = 1e-5
F32 = jnp.float32
BF16 = jnp.bfloat16
AXES = ('e', 'b', 'x', 'c')


def ein(form, *ops):
    return jnp.einsum(form, *ops, preferred_element_type=F32)


def norm_forward(x_wide, ln_gain, ln_shift):
    row_mean = jnp.mean(x_wide, axis=-1, keepdims=True)
    centered = x_wide - row_mean
    variance = jnp.mean(centered * centered, axis=-1, keepdims=True)
    inv_std = lax.rsqrt(variance + LN_EPS)
    normed = centered * inv_std
    return (normed * ln_gain + ln_shift).astype(BF16), normed, inv_std


def norm_backward(d_wide, normed, inv_std, ln_gain):
    d_normed = d_wide * ln_gain
    mean_d = jnp.mean(d_normed, axis=-1, keepdims=True)
    mean_dn = jnp.mean(d_normed * normed, axis=-1, keepdims=True)
    d_in = inv_std * (d_normed - mean_d - normed * mean_dn)
    return d_in, jnp.sum(d_wide * normed, axis=0), jnp.sum(d_wide, axis=0)


TQ = 256


def low_lanes(shape, hd):
    return lax.broadcasted_iota(jnp.int32, shape, 1) < hd


def attend_body(hd, q, k, v, ctx):
    seq, lanes = q.shape
    for t in range(seq // TQ):
        end = (t + 1) * TQ
        qt, kt, vt = q[t * TQ:end], k[:end], v[:end]
        low = low_lanes(qt.shape, hd)
        zero = jnp.zeros_like(qt)
        keep = lax.broadcasted_iota(jnp.int32, (TQ, end), 0) + t * TQ >= lax.broadcasted_iota(jnp.int32, (TQ, end), 1)
        outs = []
        for head in (0, 1):
            qh = jnp.where(low, qt, zero) if head == 0 else jnp.where(low, zero, qt)
            s = jnp.where(keep, dot(qh, kt, NT) * (hd ** -0.5), -1e30)
            s = jnp.exp(s - jnp.max(s, axis=1, keepdims=True))
            p = (s * (1.0 / jnp.sum(s, axis=1, keepdims=True))).astype(BF16)
            outs.append(dot(p, vt, NN))
        ctx[t * TQ:end] = jnp.where(low, outs[0], outs[1]).astype(BF16)


def attend(qkv, hd):
    seq, hid = qkv.shape[0], qkv.shape[1] // 3
    lanes = 2 * hd
    n = hid // lanes
    return tiled_call(functools.partial(attend_body, hd), 'attend', (n,),
                      [pl.BlockSpec((seq, lanes), lambda j, g=g: (0, g * n + j)) for g in range(3)],
                      pl.BlockSpec((seq, lanes), lambda j: (0, j)), jax.ShapeDtypeStruct((seq, hid), BF16),
                      4 * seq * seq * hid, qkv, qkv, qkv)


def attend_back_body(hd, q, k, v, dctx, dq, dk, dv, sums):
    seq, lanes = q.shape
    scale = hd ** -0.5
    acc_k = acc_v = None
    for t in range(seq // TQ):
        end = (t + 1) * TQ
        qt, dt, kt, vt = q[t * TQ:end], dctx[t * TQ:end], k[:end], v[:end]
        low = low_lanes(qt.shape, hd)
        zero = jnp.zeros_like(qt)
        keep = lax.broadcasted_iota(jnp.int32, (end, TQ), 1) + t * TQ >= lax.broadcasted_iota(jnp.int32, (end, TQ), 0)
        parts = []
        for head in (0, 1):
            qh = jnp.where(low, qt, zero) if head == 0 else jnp.where(low, zero, qt)
            dh = jnp.where(low, dt, zero) if head == 0 else jnp.where(low, zero, dt)
            s = jnp.where(keep, dot(kt, qh, NT) * scale, -1e30)
            s = jnp.exp(s - jnp.max(s, axis=0, keepdims=True))
            p = s * (1.0 / jnp.sum(s, axis=0, keepdims=True))
            dp = dot(vt, dh, NT).astype(BF16).astype(F32)
            ds = p * (dp - jnp.sum(dp * p, axis=0, keepdims=True)) * scale
            ds = ds.astype(BF16)
            parts.append((lax.dot_general(ds, kt, (((0,), (0,)), ((), ())), preferred_element_type=F32),
                          dot(ds, qt, NN), dot(p.astype(BF16), dt, NN)))
        dq[t * TQ:end] = jnp.where(low, parts[0][0], parts[1][0]).astype(BF16)
        low_k = low_lanes((end, lanes), hd)
        pk, pv = jnp.where(low_k, parts[0][1], parts[1][1]), jnp.where(low_k, parts[0][2], parts[1][2])
        if acc_k is None:
            acc_k, acc_v = pk, pv
        else:
            done = acc_k.shape[0]
            acc_k = jnp.concatenate([acc_k + pk[:done], pk[done:]], axis=0)
            acc_v = jnp.concatenate([acc_v + pv[:done], pv[done:]], axis=0)
    dk[...] = acc_k.astype(BF16)
    dv[...] = acc_v.astype(BF16)
    for g, d in enumerate((dq, dk, dv)):
        sums[g:g + 1] = jnp.sum(d[...].astype(F32), axis=0, keepdims=True)


def attend_back(qkv, d_ctx, hd):
    seq, hid = d_ctx.shape
    lanes = 2 * hd
    n = hid // lanes
    col = pl.BlockSpec((seq, lanes), lambda j: (0, j))
    o = jax.ShapeDtypeStruct((seq, hid), BF16)
    return tiled_call(functools.partial(attend_back_body, hd), 'attend_back', (n,),
                      [pl.BlockSpec((seq, lanes), lambda j, g=g: (0, g * n + j)) for g in range(3)] + [col],
                      [col, col, col, pl.BlockSpec((3, lanes), lambda j: (0, j))], [o, o, o, jax.ShapeDtypeStruct((3, hid), F32)],
                      10 * seq * seq * hid, qkv, qkv, qkv, d_ctx)


def qkv_body(h, w, bias, out):
    out[...] = (dot(h[...], w[0], NN) + bias[...]).astype(BF16)


def qkv_matmul(h, wq, bias):
    seq = h.shape[0]
    groups, hid, n = wq.shape
    per = 2
    tile = n // per
    return tiled_call(qkv_body, 'qkv', (groups, per),
                      [whole(h), pl.BlockSpec((1, hid, tile), lambda g, j: (g, 0, j)), pl.BlockSpec((1, tile), lambda g, j: (0, g * per + j))],
                      pl.BlockSpec((seq, tile), lambda g, j: (0, g * per + j)), jax.ShapeDtypeStruct((seq, groups * n), BF16),
                      2 * seq * groups * n * hid, h, wq, bias.reshape(1, groups * n))


def dh1_body(d0, d1, d2, w, dep, dh):
    p = dot(d0[...], w[0], NT)
    p += dot(d1[...], w[1], NT)
    p += dot(d2[...], w[2], NT)
    dh[...] = p.astype(BF16)


def dh1_matmul(ds, wq, dep):
    seq, n = ds[0].shape
    groups, hid, _ = wq.shape
    tile = hid // 4
    return tiled_call(dh1_body, 'dh1', (4,),
                      [whole(d) for d in ds] + [pl.BlockSpec((groups, tile, n), lambda j: (0, j, 0)), pl.BlockSpec(memory_space=pl.ANY)],
                      pl.BlockSpec((seq, tile), lambda j: (0, j)), jax.ShapeDtypeStruct((seq, hid), BF16),
                      2 * seq * groups * n * hid, *ds, wq, dep)


def gelu_tanh(pre_act):
    return jax.nn.gelu(pre_act, approximate=True)


def scatter(g):
    return lax.psum_scatter(g, ('b', 'x', 'c'), scatter_dimension=0, tiled=False)


def scatter_e(g):
    return lax.psum_scatter(g, 'e', scatter_dimension=0, tiled=False)


def matmul_t(left_t, right):
    return lax.dot_general(left_t, right, (((1,), (0,)), ((), ())), preferred_element_type=F32).astype(BF16)


def grad_cols_body(lt, r, o):
    o[...] = matmul_t(lt[...], r[...]).reshape(o.shape)


def grad_cols(left, right, ne):
    seq, rows = left.shape
    width = right.shape[1] // 8
    return pl.pallas_call(
        grad_cols_body, grid=(8,),
        in_specs=[pl.BlockSpec((rows, seq), lambda j: (0, 0)), pl.BlockSpec((seq, width), lambda j: (0, j))],
        out_specs=pl.BlockSpec((1, ne, rows // ne, width), lambda j: (j, 0, 0, 0)),
        out_shape=jax.ShapeDtypeStruct((8, ne, rows // ne, width), BF16),
        cost_estimate=pl.CostEstimate(flops=2 * seq * rows * right.shape[1], bytes_accessed=2 * rows * right.shape[1], transcendentals=0),
        name='grad_cols',
    )(left.T, right)


def grad_qkv_body(lt, r0, r1, r2, o):
    width = o.shape[-1]
    for g, r in enumerate((r0, r1, r2)):
        full = matmul_t(lt[...], r[...]).reshape(o.shape[1], o.shape[3], 2 * width)
        o[0, :, g] = full[:, :, :width]
        o[1, :, g] = full[:, :, width:]


def grad_qkv(left, rights, ne):
    seq, rows = left.shape
    width = rights[0].shape[1] // 8
    return pl.pallas_call(
        grad_qkv_body, grid=(4,),
        in_specs=[pl.BlockSpec((rows, seq), lambda j: (0, 0))] + [pl.BlockSpec((seq, 2 * width), lambda j: (0, j))] * 3,
        out_specs=pl.BlockSpec((2, ne, 3, rows // ne, width), lambda j: (j, 0, 0, 0, 0)),
        out_shape=jax.ShapeDtypeStruct((8, ne, 3, rows // ne, width), BF16),
        cost_estimate=pl.CostEstimate(flops=48 * seq * rows * width, bytes_accessed=48 * rows * width, transcendentals=0),
        name='grad_qkv',
    )(left.T, *rights)


def grad_rows_body(lt, r, o):
    full = matmul_t(lt[...], r[...]).reshape(o.shape[2], o.shape[1], o.shape[3], o.shape[4])
    for e in range(o.shape[2]):
        o[0, :, e] = full[e]


def grad_rows(left, right, ne):
    seq, rows = left.shape
    width = right.shape[1] // 2
    tile = min(width, 512)
    per = width // tile
    rr = rows // (4 * ne)
    out = pl.pallas_call(
        grad_rows_body, grid=(2, per),
        in_specs=[pl.BlockSpec((rows, seq), lambda b, n: (0, 0)), pl.BlockSpec((seq, tile), lambda b, n: (0, b * per + n))],
        out_specs=pl.BlockSpec((1, 4, ne, rr, tile), lambda b, n: (b, 0, 0, 0, n)),
        out_shape=jax.ShapeDtypeStruct((2, 4, ne, rr, width), BF16),
        cost_estimate=pl.CostEstimate(flops=2 * seq * rows * right.shape[1], bytes_accessed=2 * rows * right.shape[1], transcendentals=0),
        name='grad_rows',
    )(left.T, right)
    return out.reshape(8, ne, rr, width)


def region(kind, ref, e, h, b, x, c, width):
    if kind == 'qkv':
        return ref.at[:, e, h, :, pl.ds(pl.multiple_of((b * 4 + x * 2 + c) * width, width), width)]
    return ref.at[e, x, c, h, :, pl.ds(pl.multiple_of(b * width, width), width)]


KINDS = ('qkv', 'row')
ALLS = slice(None)


def gather_kernel(ne, *refs):
    (wq, wo, xin, evin, bvin, gq, go, xo, evo, bvo, ssem, rsem, lsem) = refs
    e, b, x, c = (lax.axis_index(ax) for ax in ('e', 'b', 'x', 'c'))
    blocks, fulls = (wq, wo), (gq, go)
    nw = len(blocks)
    widths = tuple(w.shape[-1] for w in blocks)
    mesh_id = pl.DeviceIdType.MESH
    peers = [{'e': lax.rem(e + k, ne)} for k in range(1, ne)] + [{'x': 1 - x}, {'b': 1 - b}, {'c': 1 - c}]
    barrier = pltpu.get_barrier_semaphore()
    for peer in peers:
        pl.semaphore_signal(barrier, inc=1, device_id=peer, device_id_type=mesh_id)
    pl.semaphore_wait(barrier, len(peers))

    sent = []

    def send(src, dst, peer):
        n = len(sent)
        copy = pltpu.make_async_remote_copy(src_ref=src, dst_ref=dst, send_sem=ssem.at[n], recv_sem=rsem.at[n],
                                            device_id=peer, device_id_type=mesh_id)
        copy.start()
        sent.append(copy)
        return copy

    kept = []

    def keep(src, dst):
        copy = pltpu.make_async_copy(src, dst, lsem.at[len(kept)])
        copy.start()
        kept.append(copy)
        return copy

    def to_z(src_of, dst):
        return [send(src_of(lax.rem(e + k, ne)), dst, {'e': lax.rem(e + k, ne)}) for k in range(1, ne)]

    def at(w, ee, h, bb, xx):
        return region(KINDS[w], fulls[w], ee, h, bb, xx, c, widths[w])

    def block(w):
        return blocks[w].at[...]

    cols = xin.shape[2]
    mine = pl.ds(pl.multiple_of(e * cols, cols), cols)
    z, own = {}, {}
    for w in range(nw):
        own[w] = keep(block(w), at(w, e, ALLS, b, x))
    keep(evin.at[...], evo.at[e])
    keep(bvin.at[...], bvo.at[b])
    keep(xin.at[e], xo.at[:, mine])
    waits = []
    z[0] = to_z(lambda t: block(0), at(0, e, ALLS, b, x))
    waits += to_z(lambda t: evin.at[...], evo.at[e])
    waits.append(send(bvin.at[...], bvo.at[b], {'b': 1 - b}))
    waits += to_z(lambda t: xin.at[t], xo.at[:, mine])
    for w in range(1, nw):
        z[w] = to_z(lambda t, w=w: block(w), at(w, e, ALLS, b, x))

    first, second = {}, {}
    px, pb, pc = {'x': 1 - x}, {'b': 1 - b}, {'c': 1 - c}

    def move(w, h, bb, xx, peer):
        r = at(w, ALLS, h, bb, xx)
        return send(r, r, peer)

    def after_z(w):
        own[w].wait()
        for copy in z[w]:
            copy.wait_recv()
        first[w] = [move(w, 0, b, x, px), move(w, 1, b, x, pb)]
        second[w] = [move(w, 0, b, x, pb), move(w, 1, b, x, px)]
        waits.append(move(w, ALLS, b, x, pc))

    def after_first(w):
        first[w][0].wait_recv()
        second[w].append(move(w, 0, b, 1 - x, pb))
        first[w][1].wait_recv()
        second[w].append(move(w, 1, 1 - b, x, px))
        waits.append(move(w, 0, b, 1 - x, pc))
        waits.append(move(w, 1, 1 - b, x, pc))

    def after_second(w):
        for n, (h, bb, xx) in enumerate(((0, 1 - b, x), (1, b, 1 - x), (0, 1 - b, 1 - x), (1, 1 - b, 1 - x))):
            second[w][n].wait_recv()
            waits.append(move(w, h, bb, xx, pc))

    for w in range(nw + 2):
        if w < nw:
            after_z(w)
        if 1 <= w < nw + 1:
            after_first(w - 1)
        if w >= 2:
            after_second(w - 2)
    for copy in waits:
        copy.wait_recv()
    for copy in sent:
        copy.wait_send()
    for copy in kept[nw:]:
        copy.wait()


N_SENDS = 2 * 16 + 2 * 3 + 1


def gather_all(ne, w_qkv, w_out_t, x_loc, ev, bv):
    g3, kq, nq = w_qkv.shape
    ko, no = w_out_t.shape
    seq, cols = x_loc.shape[1], x_loc.shape[2]
    s = lambda shape, dt=BF16: jax.ShapeDtypeStruct(shape, dt)
    outs = [s((g3, ne, 2, kq // 2, 8 * nq)), s((ne, 2, 2, 2, ko // 2, 2 * no)), s((seq, ne * cols)),
            s((ne,) + ev.shape, F32), s((2,) + bv.shape, F32)]
    vm = pl.BlockSpec(memory_space=pltpu.VMEM)
    hbm = pl.BlockSpec(memory_space=pl.ANY)
    gq, go, x, evo, bvo = pl.pallas_call(
        functools.partial(gather_kernel, ne),
        out_shape=outs,
        in_specs=[vm] * 5,
        out_specs=[hbm] * 5,
        scratch_shapes=[pltpu.SemaphoreType.DMA((N_SENDS,)), pltpu.SemaphoreType.DMA((N_SENDS,)), pltpu.SemaphoreType.DMA((5,))],
        compiler_params=pltpu.CompilerParams(collective_id=0, has_side_effects=True),
        name='gather_all',
    )(w_qkv.reshape(g3, 2, kq // 2, nq), w_out_t.reshape(2, ko // 2, no), x_loc, ev, bv)
    return gq.reshape(g3, ne * kq, 8 * nq), go.reshape(ne * 4 * ko, 2 * no), x, evo, bvo


NT = (((1,), (1,)), ((), ()))
NN = (((1,), (0,)), ((), ()))


def dot(left, right, dims):
    return lax.dot_general(left, right, dims, preferred_element_type=F32)


def tiled_call(body, name, grid, in_specs, out_specs, out_shape, flops, *args):
    return pl.pallas_call(body, grid=grid, in_specs=in_specs, out_specs=out_specs, out_shape=out_shape, name=name,
                          compiler_params=pltpu.CompilerParams(vmem_limit_bytes=56 * 1024 * 1024),
                          cost_estimate=pl.CostEstimate(flops=flops, bytes_accessed=flops // 256, transcendentals=0))(*args)


def whole(t):
    return pl.BlockSpec(t.shape, lambda *i: (0,) * t.ndim)


def up_body(h, w, bias, pre, act):
    p = dot(h[...], w[...].reshape(h.shape[1], -1), NN) + bias[...]
    pre[...] = p
    act[...] = gelu_tanh(p).astype(BF16)


def up_matmul(h, wu, bias):
    seq = h.shape[0]
    ne, nj, rows, width = wu.shape
    ffn = nj * width
    out = pl.BlockSpec((seq, width), lambda j: (0, j))
    return tiled_call(up_body, 'up', (nj,),
                      [whole(h), pl.BlockSpec((ne, 1, rows, width), lambda j: (0, j, 0, 0)), pl.BlockSpec((1, width), lambda j: (0, j))],
                      [out, out], [jax.ShapeDtypeStruct((seq, ffn), F32), jax.ShapeDtypeStruct((seq, ffn), BF16)],
                      2 * seq * ffn * h.shape[1], h, wu, bias.reshape(1, ffn))


def down_body(m, w, res, bias, y):
    half = w.shape[-1]
    p = res[...].astype(F32) + bias[...]
    for b in range(w.shape[1]):
        p += dot(m[:, b * half:(b + 1) * half], w[0, b].reshape(-1, half), NT)
    y[0] = p.astype(BF16)


def down_matmul(m, wd, res, bias):
    seq, ffn = m.shape
    ne, nb, xc, rows, half = wd.shape
    hid = ne * xc * rows
    tile = pl.BlockSpec((seq, xc * rows), lambda e: (0, e))
    return tiled_call(down_body, 'down', (ne,),
                      [whole(m), pl.BlockSpec((1, nb, xc, rows, half), lambda e: (e, 0, 0, 0, 0)), tile,
                       pl.BlockSpec((1, xc * rows), lambda e: (0, e))],
                      pl.BlockSpec((1, seq, xc * rows), lambda e: (e, 0, 0)), jax.ShapeDtypeStruct((ne, seq, xc * rows), BF16),
                      2 * seq * ffn * hid, m, wd, res, bias.reshape(1, hid))


GELU_A, GELU_B = 0.7978845608028654, 0.044715


def dact_body(dy, w, pre, dep0, dep1, dpre, bsum):
    width = w.shape[-1]
    d = dot(dy[...], w[...].reshape(dy.shape[1], width), NN).astype(BF16).astype(F32)
    p = pre[...]
    sq = p * p
    t = jnp.tanh(GELU_A * (p + GELU_B * (sq * p)))
    slope = 0.5 * (1.0 + t) + 0.5 * p * (1.0 - t * t) * (GELU_A * (1.0 + 3.0 * GELU_B * sq))
    d = d * slope
    bsum[...] = jnp.sum(d, axis=0, keepdims=True)
    dpre[...] = d.astype(BF16)


def dact_matmul(dy, wd, pre, *deps):
    seq, hid = dy.shape
    ne, nb, xc, rows, half = wd.shape
    ffn, tile = nb * half, min(half, 512)
    per = half // tile
    col = lambda b, n: (0, b * per + n)
    return tiled_call(dact_body, 'dact', (nb, per),
                      [whole(dy), pl.BlockSpec((ne, 1, xc, rows, tile), lambda b, n: (0, b, 0, 0, n)), pl.BlockSpec((seq, tile), col)]
                      + [pl.BlockSpec(memory_space=pl.ANY)] * 2,
                      [pl.BlockSpec((seq, tile), col), pl.BlockSpec((1, tile), col)],
                      [jax.ShapeDtypeStruct((seq, ffn), BF16), jax.ShapeDtypeStruct((1, ffn), F32)],
                      2 * seq * ffn * hid, dy, wd, pre, *deps)


def dh_body(dpre, w, dep, dh):
    width = w.shape[-1]
    p = dot(dpre[:, :width], w[0, 0], NT)
    for j in range(1, w.shape[1]):
        p += dot(dpre[:, j * width:(j + 1) * width], w[0, j], NT)
    dh[...] = p.astype(BF16)


def dh_matmul(dpre, wu, dep):
    seq, ffn = dpre.shape
    ne, nj, rows, width = wu.shape
    return tiled_call(dh_body, 'dh2', (ne,),
                      [whole(dpre), pl.BlockSpec((1, nj, rows, width), lambda e: (e, 0, 0, 0)), pl.BlockSpec(memory_space=pl.ANY)],
                      pl.BlockSpec((seq, rows), lambda e: (0, e)), jax.ShapeDtypeStruct((seq, ne * rows), BF16),
                      2 * seq * ffn * ne * rows, dpre, wu, dep)


def finish_kernel(ne, kinds, *refs):
    nm, nc = 3, len(kinds)
    mats, (xin, vin) = refs[:nm], refs[nm:nm + 2]
    outs, (xo, vout) = refs[nm + 2:2 * nm + 2], refs[2 * nm + 2:2 * nm + 4]
    scratch = refs[2 * nm + 4:]
    rc, r1, s1, r2, s2, rz, s3 = (scratch[n * nc:(n + 1) * nc] for n in range(7))
    vr, vs, ve, ssem, rsem, lsem = scratch[7 * nc:]
    e, b, x, c = (lax.axis_index(ax) for ax in ('e', 'b', 'x', 'c'))
    mesh_id = pl.DeviceIdType.MESH
    px, pb, pc = {'x': 1 - x}, {'b': 1 - b}, {'c': 1 - c}
    zs = [lax.rem(e + k, ne) for k in range(1, ne)]
    barrier = pltpu.get_barrier_semaphore()
    peers = [{'e': t} for t in zs] + [px, pb, pc]
    for peer in peers:
        pl.semaphore_signal(barrier, inc=1, device_id=peer, device_id_type=mesh_id)
    pl.semaphore_wait(barrier, len(peers))
    sent = []

    def send(src, dst, peer):
        n = len(sent)
        copy = pltpu.make_async_remote_copy(src_ref=src, dst_ref=dst, send_sem=ssem.at[n], recv_sem=rsem.at[n],
                                            device_id=peer, device_id_type=mesh_id)
        copy.start()
        sent.append(copy)
        return copy

    def piece(n, bb, xx, cc):
        mat, part = kinds[n]
        ref = mats[mat]
        return ref.at[bb, xx, cc] if part is None else ref.at[bb, xx, cc, :, part]

    def own(n, bb, xx, ee, h):
        mat, part = kinds[n]
        ref = mats[mat]
        if mat == 1:
            return ref[bb, xx, c, ee, :, h]
        return ref[bb, xx, c, ee, h] if part is None else ref[bb, xx, c, ee, part, h]

    def base(n, bb, xx, ee, h):
        got = rc[n][bb, xx, ee, :, h] if kinds[n][0] == 1 else rc[n][bb, xx, ee, h]
        return own(n, bb, xx, ee, h).astype(F32) + got.astype(F32)

    def over_e(f):
        lax.fori_loop(0, ne, lambda ee, _: (f(ee), 0)[1], 0)

    pairs = ((1 - b, 1 - x), (b, 1 - x), (1 - b, x), (b, x))
    core = [[send(piece(n, bb, xx, 1 - c), rc[n].at[bb, xx], pc) for bb, xx in pairs] for n in range(nc)]
    vec = [send(vin, vr.at[0], pc)]
    cols = xin.shape[1] // ne
    col = lambda t: pl.ds(pl.multiple_of(t * cols, cols), cols)
    keep = pltpu.make_async_copy(xin.at[:, col(e)], xo.at[e], lsem.at[0])
    keep.start()
    acts = [send(xin.at[:, col(t)], xo.at[e], {'e': t}) for t in zs]
    one, two, three = {}, {}, {}

    def stage_one(n):
        for copy in core[n]:
            copy.wait_recv()
        for i in (0, 1):
            for h in (0, 1):
                bb, xx = (i, 1 - x) if h == 0 else (1 - b, i)

                def add(ee):
                    s1[n][h, i, ee] = base(n, bb, xx, ee, h).astype(BF16)

                over_e(add)
                one[n, h, i] = send(s1[n].at[h, i], r1[n].at[h, i], px if h == 0 else pb)

    def stage_two(n):
        for i in (0, 1):
            for h in (0, 1):
                one[n, h, i].wait_recv()
        for h in (0, 1):
            bb, xx, i = (1 - b, x, 1 - b) if h == 0 else (b, 1 - x, 1 - x)

            def add(ee):
                s2[n][h, ee] = (base(n, bb, xx, ee, h) + r1[n][h, i, ee].astype(F32)).astype(BF16)

            over_e(add)
            two[n, h] = send(s2[n].at[h], r2[n].at[h], pb if h == 0 else px)

    def mine(n, h, ee):
        return base(n, b, x, ee, h) + r1[n][h, b if h == 0 else x, ee].astype(F32) + r2[n][h, ee].astype(F32)

    def stage_three(n):
        for h in (0, 1):
            two[n, h].wait_recv()
        for k, t in enumerate(zs):
            for h in (0, 1):
                s3[n][k, h] = mine(n, h, t).astype(BF16)
            three[n, k] = send(s3[n].at[k], rz[n].at[k], {'e': t})

    def stage_four(n):
        for k in range(ne - 1):
            three[n, k].wait_recv()
        mat, part = kinds[n]
        for h in (0, 1):
            acc = mine(n, h, e)
            for k in range(ne - 1):
                acc = acc + rz[n][k, h].astype(F32)
            if mat == 1:
                outs[mat][:, h] = acc.astype(BF16)
            elif part is None:
                outs[mat][h] = acc.astype(BF16)
            else:
                outs[mat][part, h] = acc.astype(BF16)

    def vec_step(step):
        vec[-1].wait_recv()
        if step < 2:
            vs[step] = (vin[...] if step == 0 else vs[0]) + vr[step]
            vec.append(send(vs.at[step], vr.at[step + 1], px if step == 0 else pb))
        else:
            ve[e] = vs[1] + vr[2]
            vec.extend(send(ve.at[e], ve.at[e], {'e': t}) for t in zs)

    for t in range(nc + 3):
        if t < nc:
            stage_one(t)
        if 1 <= t < nc + 1:
            stage_two(t - 1)
        if 2 <= t < nc + 2:
            stage_three(t - 2)
        if t >= 3:
            stage_four(t - 3)
        if 1 <= t <= 3:
            vec_step(t - 1)
    for copy in vec[3:]:
        copy.wait_recv()
    acc = ve[0]
    for t in range(1, ne):
        acc = acc + ve[t]
    vout[...] = acc
    for copy in acts:
        copy.wait_recv()
    for copy in sent:
        copy.wait_send()
    keep.wait()


def finish(ne, g_wu, g_wq, g_wo, gx, vec):
    _, _, ku, nu = g_wu.shape
    _, _, g3, kq, nq = g_wq.shape
    _, _, ko, no = g_wo.shape
    seq, hid = gx.shape
    parts = 2
    kinds = tuple((0, p) for p in range(parts)) + ((1, None), (2, None))
    u, q, o = (ku // parts // 2, nu), (g3, kq // 2, nq), (ko // 2, no)
    blocks = [u] * parts + [q, o]
    full = [(2,) + u] * parts + [(g3, 2) + q[1:], (2,) + o]
    bf = lambda *shape: pltpu.VMEM(shape, BF16)
    s = lambda *shape: jax.ShapeDtypeStruct(shape, BF16)
    vm = pl.BlockSpec(memory_space=pltpu.VMEM)
    hbm = pl.BlockSpec(memory_space=pl.ANY)
    n = 13 * len(kinds) + 3 + 3 + ne - 1
    f32 = lambda *lead: pltpu.VMEM(lead + vec.shape, F32)
    scratch = ([bf(2, 2, ne, *t) for t in full] + [bf(2, 2, ne, *t) for t in blocks] * 2 + [bf(2, ne, *t) for t in blocks] * 2
               + [bf(ne - 1, 2, *t) for t in blocks] * 2)
    ru, rq, ro, xo, vo = pl.pallas_call(
        functools.partial(finish_kernel, ne, kinds),
        out_shape=[s(parts, 2, *u), s(g3, 2, *q[1:]), s(2, *o), s(ne, seq, hid // ne), jax.ShapeDtypeStruct(vec.shape, F32)],
        in_specs=[vm] * 5,
        out_specs=[vm, vm, vm, hbm, vm],
        scratch_shapes=scratch + [f32(3), f32(2), f32(ne), pltpu.SemaphoreType.DMA((n,)), pltpu.SemaphoreType.DMA((n,)),
                                  pltpu.SemaphoreType.DMA((1,))],
        compiler_params=pltpu.CompilerParams(collective_id=1, has_side_effects=True, vmem_limit_bytes=60 * 1024 * 1024),
        name='finish',
    )(g_wu.reshape((2, 2, 2, ne, parts, 2) + u), g_wq.reshape((2, 2, 2, ne, g3, 2) + q[1:]), g_wo.reshape((2, 2, 2, ne, 2) + o), gx, vec)
    return ru.reshape(ku, nu), rq.reshape(g3, kq, nq), ro.reshape(ko, no), xo, vo


def solution(mesh):
    ne, nb = mesh.shape['e'], mesh.shape['b']
    fine = Mesh(mesh.devices.reshape(ne, nb, 2, 2), ('e', 'b', 'x', 'c'))
    spec_act = P(('x', 'c', 'b'), None, 'e')
    spec_e = P('e')
    spec_b = P('b')
    spec_qkv = P(None, 'e', ('b', 'x', 'c'))
    spec_qkv_bias = P(None, 'b', None)
    spec_rows_b = P('b', ('e', 'x', 'c'))
    spec_rows_e = P('e', ('b', 'x', 'c'))
    all_specs = (spec_act, spec_act, spec_e, spec_e, spec_qkv, spec_qkv_bias, spec_rows_b,
                 spec_e, spec_e, spec_e, spec_rows_e, spec_b, spec_rows_b, spec_e)

    def local_step(x_loc, dy_loc, ln1_gain, ln1_shift, w_qkv, b_qkv, w_out, b_out, ln2_gain, ln2_shift, w_up, b_up, w_down, b_down):
        seq, cols = x_loc.shape[1], x_loc.shape[2]
        hid = cols * ne
        heads, hd = b_qkv.shape[1] * nb, b_qkv.shape[2]
        ffn = b_up.shape[0] * nb
        hl = hid // nb
        ix = {ax: lax.axis_index(ax) for ax in ('e', 'b', 'x', 'c')}

        ev = jnp.stack([ln1_gain, ln1_shift, b_out, ln2_gain, ln2_shift, b_down])
        bv = jnp.concatenate([b_qkv.reshape(-1), b_up]).reshape(-1, 128)
        wu = lax.all_gather(w_up, AXES, axis=0, tiled=False).reshape((ne, 8) + w_up.shape)
        wd = lax.all_gather(w_down.T, AXES, axis=0, tiled=False).reshape((ne, 2, 4) + w_down.T.shape)
        wq, wo, x, ev, bv = gather_all(ne, w_qkv, w_out.T, x_loc, ev, bv)
        dy_loc, x = lax.optimization_barrier((dy_loc, x))
        dy = lax.all_to_all(dy_loc, 'e', split_axis=0, concat_axis=0, tiled=True).transpose(1, 0, 2).reshape(seq, hid)
        x = x.astype(F32)
        ev = ev.transpose(1, 0, 2).reshape(6, hid)
        ln1_g, ln1_s, bo, ln2_g, ln2_s, bd = [ev[i] for i in range(6)]
        bv = bv.reshape(nb, -1)
        bq = bv[:, :3 * hl].reshape(nb, 3, hl).transpose(1, 0, 2).reshape(3, hid)
        bu = bv[:, 3 * hl:].reshape(ffn)

        h1, n1, i1 = norm_forward(x, ln1_g, ln1_s)
        qkv = qkv_matmul(h1, wq, bq)
        ctx = attend(qkv, hd)
        x1 = (x + ein('sk,nk->sn', ctx, wo) + bo).astype(BF16)
        h2, n2, i2 = norm_forward(x1.astype(F32), ln2_g, ln2_s)
        pre, m = up_matmul(h2, wu, bu)
        g_wd_blocks = grad_rows(dy, m, ne)
        g_wd = scatter(g_wd_blocks)
        y = down_matmul(m, wd, x1, bd)
        y_loc = lax.all_to_all(y, 'e', split_axis=0, concat_axis=0, tiled=True)

        dyf = dy.astype(F32)
        g_bd = jnp.sum(dyf, axis=0)
        d_pre, g_bu = dact_matmul(dy, wd, pre, g_wd_blocks, y)
        g_bu = g_bu[0]
        g_wu_blocks = grad_cols(h2, d_pre, ne)
        d_h2 = dh_matmul(d_pre, wu, g_wu_blocks)
        d_n2, g_g2, g_s2 = norm_backward(d_h2.astype(F32), n2, i2, ln2_g)
        d_x1 = (dyf + d_n2).astype(BF16)
        d_x1f = d_x1.astype(F32)
        g_bo = jnp.sum(d_x1f, axis=0)
        g_wo = grad_rows(d_x1, ctx, ne)
        d_ctx = ein('sn,nk->sk', d_x1, wo).astype(BF16)
        *d_qkv, g_bq = attend_back(qkv, d_ctx, hd)
        g_bq = g_bq.reshape(-1)
        g_wq = grad_qkv(h1, d_qkv, ne)
        d_h1 = dh1_matmul(d_qkv, wq, y_loc)
        d_n1, g_g1, g_s1 = norm_backward(d_h1.astype(F32), n1, i1, ln1_g)
        g_wd, g_wq, g_wo = lax.optimization_barrier((g_wd, g_wq, g_wo))
        g_wd = scatter_e(g_wd)
        vec = jnp.concatenate([g_bo, g_g2, g_s2, g_bd, g_bq, g_bu, g_g1, g_s1]).reshape(-1, 128)
        g_wu, g_wq, g_wo, gx_loc, vec = finish(ne, g_wu_blocks, g_wq, g_wo, (d_x1f + d_n1).astype(BF16), vec)
        vec = vec.reshape(-1)
        early, late = vec[:7 * hid + ffn], vec[7 * hid + ffn:]

        cut_e = lambda v: lax.dynamic_slice_in_dim(v, ix['e'] * cols, cols)
        r_bo, r_g2, r_s2, r_bd = [cut_e(early[i * hid:(i + 1) * hid]) for i in range(4)]
        r_bq = lax.dynamic_slice_in_dim(early[4 * hid:7 * hid].reshape(3, heads, hd), ix['b'] * (heads // nb), heads // nb, axis=1)
        r_bu = lax.dynamic_slice_in_dim(early[7 * hid:], ix['b'] * (ffn // nb), ffn // nb)
        r_g1, r_s1 = cut_e(late[:hid]), cut_e(late[hid:])
        return (y_loc, gx_loc, r_g1, r_s1, g_wq, r_bq, g_wo.T, r_bo,
                r_g2, r_s2, g_wu, r_bu, g_wd.T, r_bd)

    return jax.shard_map(local_step, mesh=fine, in_specs=all_specs, out_specs=all_specs, check_vma=False)
```

```python
import functools

import jax
import jax.numpy as jnp
from jax import lax
from jax.experimental import pallas as pl
from jax.experimental.pallas import tpu as pltpu
from jax.sharding import Mesh, PartitionSpec as P

LN_EPS = 1e-5
F32 = jnp.float32
BF16 = jnp.bfloat16
AXES = ('e', 'b', 'x', 'c')
HALVES = range(2)
TN = (((0,), (0,)), ((), ()))
NT = (((1,), (1,)), ((), ()))
NN = (((1,), (0,)), ((), ()))


def ein(form, *ops):
    return jnp.einsum(form, *ops, preferred_element_type=F32)


def norm_forward(x_wide, ln_gain, ln_shift):
    row_mean = jnp.mean(x_wide, axis=-1, keepdims=True)
    centered = x_wide - row_mean
    variance = jnp.mean(centered * centered, axis=-1, keepdims=True)
    inv_std = lax.rsqrt(variance + LN_EPS)
    normed = centered * inv_std
    return (normed * ln_gain + ln_shift).astype(BF16), normed, inv_std


def norm_backward(d_wide, normed, inv_std, ln_gain):
    d_normed = d_wide * ln_gain
    mean_d = jnp.mean(d_normed, axis=-1, keepdims=True)
    mean_dn = jnp.mean(d_normed * normed, axis=-1, keepdims=True)
    d_in = inv_std * (d_normed - mean_d - normed * mean_dn)
    return d_in, jnp.sum(d_wide * normed, axis=0), jnp.sum(d_wide, axis=0)


TQ = 256


def low_lanes(shape, hd):
    return lax.broadcasted_iota(jnp.int32, shape, 1) < hd


def attend_body(hd, q, k, v, ctx):
    seq, lanes = q.shape
    for t in range(seq // TQ):
        end = (t + 1) * TQ
        qt, kt, vt = q[t * TQ:end], k[:end], v[:end]
        low = low_lanes(qt.shape, hd)
        zero = jnp.zeros_like(qt)
        keep = lax.broadcasted_iota(jnp.int32, (TQ, end), 0) + t * TQ >= lax.broadcasted_iota(jnp.int32, (TQ, end), 1)
        outs = []
        for head in HALVES:
            qh = jnp.where(low, qt, zero) if head == 0 else jnp.where(low, zero, qt)
            s = jnp.where(keep, dot(qh, kt, NT) * (hd ** -0.5), -1e30)
            s = jnp.exp(s - jnp.max(s, axis=1, keepdims=True))
            p = (s * (1.0 / jnp.sum(s, axis=1, keepdims=True))).astype(BF16)
            outs.append(dot(p, vt, NN))
        ctx[t * TQ:end] = jnp.where(low, outs[0], outs[1]).astype(BF16)


def attend(qkv, hd):
    seq, hid = qkv.shape[0], qkv.shape[1] // 3
    lanes = 2 * hd
    n = hid // lanes
    return tiled_call(functools.partial(attend_body, hd), 'attend', (n,),
                      [cols_of(seq, lanes, g * n) for g in range(3)], cols_of(seq, lanes), jax.ShapeDtypeStruct((seq, hid), BF16),
                      4 * seq * seq * hid, qkv, qkv, qkv)


def down_sum(t):
    return jnp.sum(t, axis=0, keepdims=True)


def down_max(t):
    return jnp.max(t, axis=0, keepdims=True)


def attend_back_body(hd, q, k, v, dctx, dq, dk, dv, sums):
    seq, lanes = q.shape
    scale = hd ** -0.5
    acc_k = acc_v = None
    for t in range(seq // TQ):
        end = (t + 1) * TQ
        qt, dt, kt, vt = q[t * TQ:end], dctx[t * TQ:end], k[:end], v[:end]
        low = low_lanes(qt.shape, hd)
        zero = jnp.zeros_like(qt)
        keep = lax.broadcasted_iota(jnp.int32, (end, TQ), 1) + t * TQ >= lax.broadcasted_iota(jnp.int32, (end, TQ), 0)
        parts = []
        for head in HALVES:
            qh = jnp.where(low, qt, zero) if head == 0 else jnp.where(low, zero, qt)
            dh = jnp.where(low, dt, zero) if head == 0 else jnp.where(low, zero, dt)
            s = jnp.where(keep, dot(kt, qh, NT) * scale, -1e30)
            s = jnp.exp(s - down_max(s))
            p = s * (1.0 / down_sum(s))
            dp = dot(vt, dh, NT).astype(BF16).astype(F32)
            ds = p * (dp - down_sum(dp * p)) * scale
            ds = ds.astype(BF16)
            parts.append((dot(ds, kt, TN),
                          dot(ds, qt, NN), dot(p.astype(BF16), dt, NN)))
        (q0, k0, v0), (q1, k1, v1) = parts
        dq[t * TQ:end] = jnp.where(low, q0, q1).astype(BF16)
        low_k = low_lanes((end, lanes), hd)
        pk, pv = jnp.where(low_k, k0, k1), jnp.where(low_k, v0, v1)
        if acc_k is None:
            acc_k, acc_v = pk, pv
        else:
            done = acc_k.shape[0]
            acc_k = jnp.concatenate([acc_k + pk[:done], pk[done:]], axis=0)
            acc_v = jnp.concatenate([acc_v + pv[:done], pv[done:]], axis=0)
    dk[...] = acc_k.astype(BF16)
    dv[...] = acc_v.astype(BF16)
    for g, d in enumerate((dq, dk, dv)):
        sums[g:g + 1] = down_sum(d[...].astype(F32))


def attend_back(qkv, d_ctx, hd):
    seq, hid = d_ctx.shape
    lanes = 2 * hd
    n = hid // lanes
    col = cols_of(seq, lanes)
    o = jax.ShapeDtypeStruct((seq, hid), BF16)
    return tiled_call(functools.partial(attend_back_body, hd), 'attend_back', (n,),
                      [cols_of(seq, lanes, g * n) for g in range(3)] + [col],
                      [col, col, col, cols_of(3, lanes)], [o, o, o, jax.ShapeDtypeStruct((3, hid), F32)],
                      10 * seq * seq * hid, qkv, qkv, qkv, d_ctx)


def qkv_body(h, w, bias, out):
    out[...] = (dot(h[...], w[0], NN) + bias[...]).astype(BF16)


def qkv_matmul(h, wq, bias):
    seq = h.shape[0]
    groups, hid, n = wq.shape
    per = 2
    tile = n // per
    return tiled_call(qkv_body, 'qkv', (groups, per),
                      [whole(h), pl.BlockSpec((1, hid, tile), lambda g, j: (g, 0, j)), pl.BlockSpec((1, tile), lambda g, j: (0, g * per + j))],
                      pl.BlockSpec((seq, tile), lambda g, j: (0, g * per + j)), jax.ShapeDtypeStruct((seq, groups * n), BF16),
                      2 * seq * groups * n * hid, h, wq, bias.reshape(1, groups * n))


def dh1_body(d0, d1, d2, w, dep, dh):
    dh[...] = sum(dot(d[...], w[g], NT) for g, d in enumerate((d0, d1, d2))).astype(BF16)


def dh1_matmul(ds, wq, dep):
    seq, n = ds[0].shape
    groups, hid, _ = wq.shape
    tile = hid // 4
    return tiled_call(dh1_body, 'dh1', (4,),
                      [whole(d) for d in ds] + [pl.BlockSpec((groups, tile, n), lambda j: (0, j, 0)), pl.BlockSpec(memory_space=pl.ANY)],
                      cols_of(seq, tile), jax.ShapeDtypeStruct((seq, hid), BF16),
                      2 * seq * groups * n * hid, *ds, wq, dep)


def gelu_tanh(pre_act):
    return jax.nn.gelu(pre_act, approximate=True)


def scatter(g):
    return lax.psum_scatter(g, AXES[1:])


def swap_e(t):
    return lax.all_to_all(t, 'e', split_axis=0, concat_axis=0, tiled=True)


def scatter_e(g):
    return lax.psum_scatter(g, 'e')


def matmul_t(left_t, right):
    return dot(left_t, right, NN).astype(BF16)


def grad_cols_body(lt, r, o):
    o[...] = matmul_t(lt[...], r[...]).reshape(o.shape)


def grad_cols(left, right, ne):
    seq, rows = left.shape
    width = right.shape[1] // 8
    return tiled_call(grad_cols_body, 'grad_cols', (8,), [whole(left.T), cols_of(seq, width)],
                      pl.BlockSpec((1, ne, rows // ne, width), lambda j: (j, 0, 0, 0)),
                      jax.ShapeDtypeStruct((8, ne, rows // ne, width), BF16), 16 * seq * rows * width, left.T, right)


def grad_qkv_body(lt, r0, r1, r2, o):
    width = o.shape[-1]
    for g, r in enumerate((r0, r1, r2)):
        full = matmul_t(lt[...], r[...]).reshape(o.shape[1], o.shape[3], 2 * width)
        o[0, :, g] = full[:, :, :width]
        o[1, :, g] = full[:, :, width:]


def grad_qkv(left, rights, ne):
    seq, rows = left.shape
    width = rights[0].shape[1] // 8
    return tiled_call(grad_qkv_body, 'grad_qkv', (4,), [whole(left.T)] + [cols_of(seq, 2 * width)] * 3,
                      pl.BlockSpec((2, ne, 3, rows // ne, width), lambda j: (j, 0, 0, 0, 0)),
                      jax.ShapeDtypeStruct((8, ne, 3, rows // ne, width), BF16), 48 * seq * rows * width, left.T, *rights)


def grad_rows_body(lt, r, o):
    full = matmul_t(lt[...], r[...]).reshape(o.shape[2], o.shape[1], o.shape[3], o.shape[4])
    for e in range(o.shape[2]):
        o[0, :, e] = full[e]


def grad_rows(left, right, ne):
    seq, rows = left.shape
    width = right.shape[1] // 2
    tile = min(width, 512)
    per = width // tile
    rr = rows // (4 * ne)
    out = tiled_call(grad_rows_body, 'grad_rows', (2 * per,), [whole(left.T), cols_of(seq, tile)],
                     pl.BlockSpec((1, 4, ne, rr, tile), lambda j: (j // per, 0, 0, 0, j % per)),
                     jax.ShapeDtypeStruct((2, 4, ne, rr, width), BF16), 4 * seq * rows * width, left.T, right)
    return out.reshape(8, ne, rr, width)


def region(kind, ref, e, h, b, x, c, width):
    if kind == 'qkv':
        return ref.at[:, e, h, :, pl.ds(pl.multiple_of((b * 4 + x * 2 + c) * width, width), width)]
    return ref.at[e, x, c, h, :, pl.ds(pl.multiple_of(b * width, width), width)]


KINDS = ('qkv', 'row')
ALLS = slice(None)


def gather_kernel(ne, *refs):
    (wq, wo, xin, evin, bvin, gq, go, xo, evo, bvo, ssem, rsem, lsem) = refs
    e, b, x, c = (lax.axis_index(ax) for ax in AXES)
    ob, ox, oc = (1 - t for t in (b, x, c))
    px, pb, pc = {'x': ox}, {'b': ob}, {'c': oc}
    blocks, fulls = (wq, wo), (gq, go)
    nw = len(blocks)
    widths = tuple(w.shape[-1] for w in blocks)
    mesh_id = pl.DeviceIdType.MESH
    peers = [{'e': lax.rem(e + k, ne)} for k in range(1, ne)] + [px, pb, pc]
    barrier = pltpu.get_barrier_semaphore()
    for peer in peers:
        pl.semaphore_signal(barrier, inc=1, device_id=peer, device_id_type=mesh_id)
    pl.semaphore_wait(barrier, len(peers))

    sent = []

    def send(src, dst, peer):
        n = len(sent)
        copy = pltpu.make_async_remote_copy(src_ref=src, dst_ref=dst, send_sem=ssem.at[n], recv_sem=rsem.at[n],
                                            device_id=peer, device_id_type=mesh_id)
        copy.start()
        sent.append(copy)
        return copy

    kept = []

    def keep(src, dst):
        copy = pltpu.make_async_copy(src, dst, lsem.at[len(kept)])
        copy.start()
        kept.append(copy)
        return copy

    def to_z(src_of, dst):
        return [send(src_of(lax.rem(e + k, ne)), dst, {'e': lax.rem(e + k, ne)}) for k in range(1, ne)]

    def at(w, ee, h, bb, xx):
        return region(KINDS[w], fulls[w], ee, h, bb, xx, c, widths[w])

    def block(w):
        return blocks[w].at[...]

    cols = xin.shape[2]
    mine = pl.ds(pl.multiple_of(e * cols, cols), cols)
    z, own = {}, {}
    for w in range(nw):
        own[w] = keep(block(w), at(w, e, ALLS, b, x))
    keep(evin.at[...], evo.at[e])
    keep(bvin.at[...], bvo.at[b])
    keep(xin.at[e], xo.at[:, mine])
    waits = []
    z[0] = to_z(lambda t: block(0), at(0, e, ALLS, b, x))
    waits += to_z(lambda t: evin.at[...], evo.at[e])
    waits.append(send(bvin.at[...], bvo.at[b], pb))
    waits += to_z(lambda t: xin.at[t], xo.at[:, mine])
    for w in range(1, nw):
        z[w] = to_z(lambda t, w=w: block(w), at(w, e, ALLS, b, x))

    first, second = {}, {}

    def move(w, h, bb, xx, peer):
        r = at(w, ALLS, h, bb, xx)
        return send(r, r, peer)

    def after_z(w):
        own[w].wait()
        for copy in z[w]:
            copy.wait_recv()
        first[w] = [move(w, 0, b, x, px), move(w, 1, b, x, pb)]
        second[w] = [move(w, 0, b, x, pb), move(w, 1, b, x, px)]
        waits.append(move(w, ALLS, b, x, pc))

    def after_first(w):
        first[w][0].wait_recv()
        second[w].append(move(w, 0, b, ox, pb))
        first[w][1].wait_recv()
        second[w].append(move(w, 1, ob, x, px))
        waits.append(move(w, 0, b, ox, pc))
        waits.append(move(w, 1, ob, x, pc))

    def after_second(w):
        for n, (h, bb, xx) in enumerate(((0, ob, x), (1, b, ox), (0, ob, ox), (1, ob, ox))):
            second[w][n].wait_recv()
            waits.append(move(w, h, bb, xx, pc))

    for w in range(nw + 2):
        if w < nw:
            after_z(w)
        if 1 <= w < nw + 1:
            after_first(w - 1)
        if w >= 2:
            after_second(w - 2)
    for copy in waits:
        copy.wait_recv()
    for copy in sent:
        copy.wait_send()
    for copy in kept[nw:]:
        copy.wait()


N_SENDS = 2 * 16 + 2 * 3 + 1


def gather_all(ne, w_qkv, w_out_t, x_loc, ev, bv):
    g3, kq, nq = w_qkv.shape
    ko, no = w_out_t.shape
    seq, cols = x_loc.shape[1], x_loc.shape[2]
    s = lambda shape, dt=BF16: jax.ShapeDtypeStruct(shape, dt)
    outs = [s((g3, ne, 2, kq // 2, 8 * nq)), s((ne, 2, 2, 2, ko // 2, 2 * no)), s((seq, ne * cols)),
            s((ne,) + ev.shape, F32), s((2,) + bv.shape, F32)]
    vm = pl.BlockSpec(memory_space=pltpu.VMEM)
    hbm = pl.BlockSpec(memory_space=pl.ANY)
    gq, go, x, evo, bvo = pl.pallas_call(
        functools.partial(gather_kernel, ne),
        out_shape=outs,
        in_specs=[vm] * 5,
        out_specs=[hbm] * 5,
        scratch_shapes=[pltpu.SemaphoreType.DMA((N_SENDS,)), pltpu.SemaphoreType.DMA((N_SENDS,)), pltpu.SemaphoreType.DMA((5,))],
        compiler_params=pltpu.CompilerParams(collective_id=0, has_side_effects=True),
        name='gather_all',
    )(w_qkv.reshape(g3, 2, kq // 2, nq), w_out_t.reshape(2, ko // 2, no), x_loc, ev, bv)
    return gq.reshape(g3, ne * kq, 8 * nq), go.reshape(ne * 4 * ko, 2 * no), x, evo, bvo


def dot(left, right, dims):
    return lax.dot_general(left, right, dims, preferred_element_type=F32)


def tiled_call(body, name, grid, in_specs, out_specs, out_shape, flops, *args):
    return pl.pallas_call(body, grid=grid, in_specs=in_specs, out_specs=out_specs, out_shape=out_shape, name=name,
                          compiler_params=pltpu.CompilerParams(vmem_limit_bytes=56 * 1024 * 1024),
                          cost_estimate=pl.CostEstimate(flops=flops, bytes_accessed=flops // 256, transcendentals=0))(*args)


def whole(t):
    return pl.BlockSpec(t.shape, lambda *i: (0,) * t.ndim)


def cols_of(rows, width, start=0):
    return pl.BlockSpec((rows, width), lambda j: (0, start + j))


def up_body(h, w, bias, pre, act):
    p = dot(h[...], w[...].reshape(h.shape[1], -1), NN) + bias[...]
    pre[...] = p
    act[...] = gelu_tanh(p).astype(BF16)


def up_matmul(h, wu, bias):
    seq = h.shape[0]
    ne, nj, rows, width = wu.shape
    ffn = nj * width
    out = cols_of(seq, width)
    return tiled_call(up_body, 'up', (nj,),
                      [whole(h), pl.BlockSpec((ne, 1, rows, width), lambda j: (0, j, 0, 0)), cols_of(1, width)],
                      [out, out], [jax.ShapeDtypeStruct((seq, ffn), F32), jax.ShapeDtypeStruct((seq, ffn), BF16)],
                      2 * seq * ffn * h.shape[1], h, wu, bias.reshape(1, ffn))


def down_body(m, w, res, bias, y):
    half = w.shape[-1]
    p = res[...].astype(F32) + bias[...]
    for b in range(w.shape[1]):
        p += dot(m[:, b * half:(b + 1) * half], w[0, b].reshape(-1, half), NT)
    y[0] = p.astype(BF16)


def down_matmul(m, wd, res, bias):
    seq, ffn = m.shape
    ne, nb, xc, rows, half = wd.shape
    hid = ne * xc * rows
    tile = cols_of(seq, xc * rows)
    return tiled_call(down_body, 'down', (ne,),
                      [whole(m), pl.BlockSpec((1, nb, xc, rows, half), lambda e: (e, 0, 0, 0, 0)), tile,
                       cols_of(1, xc * rows)],
                      pl.BlockSpec((1, seq, xc * rows), lambda e: (e, 0, 0)), jax.ShapeDtypeStruct((ne, seq, xc * rows), BF16),
                      2 * seq * ffn * hid, m, wd, res, bias.reshape(1, hid))


GELU_A, GELU_B = 0.7978845608028654, 0.044715


def dact_body(dy, w, pre, dep0, dep1, dpre, bsum):
    width = w.shape[-1]
    d = dot(dy[...], w[...].reshape(dy.shape[1], width), NN).astype(BF16).astype(F32)
    p = pre[...]
    sq = p * p
    t = jnp.tanh(GELU_A * (p + GELU_B * (sq * p)))
    slope = 0.5 * (1.0 + t) + 0.5 * p * (1.0 - t * t) * (GELU_A * (1.0 + 3.0 * GELU_B * sq))
    d = d * slope
    bsum[...] = down_sum(d)
    dpre[...] = d.astype(BF16)


def dact_matmul(dy, wd, pre, *deps):
    seq, hid = dy.shape
    ne, nb, xc, rows, half = wd.shape
    ffn, tile = nb * half, min(half, 512)
    per = half // tile
    col = lambda b, n: (0, b * per + n)
    return tiled_call(dact_body, 'dact', (nb, per),
                      [whole(dy), pl.BlockSpec((ne, 1, xc, rows, tile), lambda b, n: (0, b, 0, 0, n)), pl.BlockSpec((seq, tile), col)]
                      + [pl.BlockSpec(memory_space=pl.ANY)] * 2,
                      [pl.BlockSpec((seq, tile), col), pl.BlockSpec((1, tile), col)],
                      [jax.ShapeDtypeStruct((seq, ffn), BF16), jax.ShapeDtypeStruct((1, ffn), F32)],
                      2 * seq * ffn * hid, dy, wd, pre, *deps)


def dh_body(dpre, w, dep, dh):
    width = w.shape[-1]
    dh[...] = sum(dot(dpre[:, j * width:(j + 1) * width], w[0, j], NT) for j in range(w.shape[1])).astype(BF16)


def dh_matmul(dpre, wu, dep):
    seq, ffn = dpre.shape
    ne, nj, rows, width = wu.shape
    return tiled_call(dh_body, 'dh2', (ne,),
                      [whole(dpre), pl.BlockSpec((1, nj, rows, width), lambda e: (e, 0, 0, 0)), pl.BlockSpec(memory_space=pl.ANY)],
                      cols_of(seq, rows), jax.ShapeDtypeStruct((seq, ne * rows), BF16),
                      2 * seq * ffn * ne * rows, dpre, wu, dep)


def finish_kernel(ne, kinds, *refs):
    nm, nc = 3, len(kinds)
    mats, (xin, vin) = refs[:nm], refs[nm:nm + 2]
    outs, (xo, vout) = refs[nm + 2:2 * nm + 2], refs[2 * nm + 2:2 * nm + 4]
    scratch = refs[2 * nm + 4:]
    rc, r1, s1, r2, s2, rz, s3 = (scratch[n * nc:(n + 1) * nc] for n in range(7))
    vr, vs, ve, ssem, rsem, lsem = scratch[7 * nc:]
    e, b, x, c = (lax.axis_index(ax) for ax in AXES)
    ob, ox, oc = (1 - t for t in (b, x, c))
    mesh_id = pl.DeviceIdType.MESH
    px, pb, pc = {'x': ox}, {'b': ob}, {'c': oc}
    zs = [lax.rem(e + k, ne) for k in range(1, ne)]
    barrier = pltpu.get_barrier_semaphore()
    peers = [{'e': t} for t in zs] + [px, pb, pc]
    for peer in peers:
        pl.semaphore_signal(barrier, inc=1, device_id=peer, device_id_type=mesh_id)
    pl.semaphore_wait(barrier, len(peers))
    sent = []

    def send(src, dst, peer):
        n = len(sent)
        copy = pltpu.make_async_remote_copy(src_ref=src, dst_ref=dst, send_sem=ssem.at[n], recv_sem=rsem.at[n],
                                            device_id=peer, device_id_type=mesh_id)
        copy.start()
        sent.append(copy)
        return copy

    def piece(n, bb, xx, cc):
        mat, part = kinds[n]
        ref = mats[mat]
        return ref.at[bb, xx, cc] if part is None else ref.at[bb, xx, cc, :, part]

    def own(n, bb, xx, ee, h):
        mat, part = kinds[n]
        ref = mats[mat]
        if mat == 1:
            return ref[bb, xx, c, ee, :, h]
        return ref[bb, xx, c, ee, h] if part is None else ref[bb, xx, c, ee, part, h]

    def base(n, bb, xx, ee, h):
        got = rc[n][bb, xx, ee, :, h] if kinds[n][0] == 1 else rc[n][bb, xx, ee, h]
        return own(n, bb, xx, ee, h).astype(F32) + got.astype(F32)

    def over_e(f):
        lax.fori_loop(0, ne, lambda ee, _: (f(ee), 0)[1], 0)

    pairs = ((ob, ox), (b, ox), (ob, x), (b, x))
    core = [[send(piece(n, bb, xx, oc), rc[n].at[bb, xx], pc) for bb, xx in pairs] for n in range(nc)]
    vec = [send(vin, vr.at[0], pc)]
    cols = xin.shape[1] // ne
    col = lambda t: pl.ds(pl.multiple_of(t * cols, cols), cols)
    keep = pltpu.make_async_copy(xin.at[:, col(e)], xo.at[e], lsem.at[0])
    keep.start()
    acts = [send(xin.at[:, col(t)], xo.at[e], {'e': t}) for t in zs]
    one, two, three = {}, {}, {}

    def stage_one(n):
        for copy in core[n]:
            copy.wait_recv()
        for i in HALVES:
            for h in HALVES:
                bb, xx = (i, ox) if h == 0 else (ob, i)

                def add(ee):
                    s1[n][h, i, ee] = base(n, bb, xx, ee, h).astype(BF16)

                over_e(add)
                one[n, h, i] = send(s1[n].at[h, i], r1[n].at[h, i], px if h == 0 else pb)

    def stage_two(n):
        for i in HALVES:
            for h in HALVES:
                one[n, h, i].wait_recv()
        for h in HALVES:
            bb, xx, i = (ob, x, ob) if h == 0 else (b, ox, ox)

            def add(ee):
                s2[n][h, ee] = (base(n, bb, xx, ee, h) + r1[n][h, i, ee].astype(F32)).astype(BF16)

            over_e(add)
            two[n, h] = send(s2[n].at[h], r2[n].at[h], pb if h == 0 else px)

    def mine(n, h, ee):
        return base(n, b, x, ee, h) + r1[n][h, b if h == 0 else x, ee].astype(F32) + r2[n][h, ee].astype(F32)

    def stage_three(n):
        for h in HALVES:
            two[n, h].wait_recv()
        for k, t in enumerate(zs):
            for h in HALVES:
                s3[n][k, h] = mine(n, h, t).astype(BF16)
            three[n, k] = send(s3[n].at[k], rz[n].at[k], {'e': t})

    def stage_four(n):
        for k in range(ne - 1):
            three[n, k].wait_recv()
        mat, part = kinds[n]
        for h in HALVES:
            acc = mine(n, h, e)
            for k in range(ne - 1):
                acc = acc + rz[n][k, h].astype(F32)
            if mat == 1:
                outs[mat][:, h] = acc.astype(BF16)
            elif part is None:
                outs[mat][h] = acc.astype(BF16)
            else:
                outs[mat][part, h] = acc.astype(BF16)

    def vec_step(step):
        vec[-1].wait_recv()
        if step < 2:
            vs[step] = (vin[...] if step == 0 else vs[0]) + vr[step]
            vec.append(send(vs.at[step], vr.at[step + 1], px if step == 0 else pb))
        else:
            ve[e] = vs[1] + vr[2]
            vec.extend(send(ve.at[e], ve.at[e], {'e': t}) for t in zs)

    for t in range(nc + 3):
        if t < nc:
            stage_one(t)
        if 1 <= t < nc + 1:
            stage_two(t - 1)
        if 2 <= t < nc + 2:
            stage_three(t - 2)
        if t >= 3:
            stage_four(t - 3)
        if 1 <= t <= 3:
            vec_step(t - 1)
    for copy in vec[3:]:
        copy.wait_recv()
    acc = ve[0]
    for t in range(1, ne):
        acc = acc + ve[t]
    vout[...] = acc
    for copy in acts:
        copy.wait_recv()
    for copy in sent:
        copy.wait_send()
    keep.wait()


def finish(ne, g_wu, g_wq, g_wo, gx, vec):
    _, _, ku, nu = g_wu.shape
    _, _, g3, kq, nq = g_wq.shape
    _, _, ko, no = g_wo.shape
    seq, hid = gx.shape
    parts = 2
    kinds = tuple((0, p) for p in range(parts)) + ((1, None), (2, None))
    u, q, o = (ku // parts // 2, nu), (g3, kq // 2, nq), (ko // 2, no)
    blocks = [u] * parts + [q, o]
    full = [(2,) + u] * parts + [(g3, 2) + q[1:], (2,) + o]
    bf = lambda *shape: pltpu.VMEM(shape, BF16)
    s = lambda *shape: jax.ShapeDtypeStruct(shape, BF16)
    vm = pl.BlockSpec(memory_space=pltpu.VMEM)
    hbm = pl.BlockSpec(memory_space=pl.ANY)
    n = 13 * len(kinds) + 3 + 3 + ne - 1
    f32 = lambda *lead: pltpu.VMEM(lead + vec.shape, F32)
    scratch = ([bf(2, 2, ne, *t) for t in full] + [bf(2, 2, ne, *t) for t in blocks] * 2 + [bf(2, ne, *t) for t in blocks] * 2
               + [bf(ne - 1, 2, *t) for t in blocks] * 2)
    ru, rq, ro, xo, vo = pl.pallas_call(
        functools.partial(finish_kernel, ne, kinds),
        out_shape=[s(parts, 2, *u), s(g3, 2, *q[1:]), s(2, *o), s(ne, seq, hid // ne), jax.ShapeDtypeStruct(vec.shape, F32)],
        in_specs=[vm] * 5,
        out_specs=[vm, vm, vm, hbm, vm],
        scratch_shapes=scratch + [f32(3), f32(2), f32(ne), pltpu.SemaphoreType.DMA((n,)), pltpu.SemaphoreType.DMA((n,)),
                                  pltpu.SemaphoreType.DMA((1,))],
        compiler_params=pltpu.CompilerParams(collective_id=1, has_side_effects=True, vmem_limit_bytes=60 * 1024 * 1024),
        name='finish',
    )(g_wu.reshape((2, 2, 2, ne, parts, 2) + u), g_wq.reshape((2, 2, 2, ne, g3, 2) + q[1:]), g_wo.reshape((2, 2, 2, ne, 2) + o), gx, vec)
    return ru.reshape(ku, nu), rq.reshape(g3, kq, nq), ro.reshape(ko, no), xo, vo


def solution(mesh):
    ne, nb = mesh.shape['e'], mesh.shape['b']
    fine = Mesh(mesh.devices.reshape(ne, nb, 2, 2), ('e', 'b', 'x', 'c'))
    spec_act = P(('x', 'c', 'b'), None, 'e')
    spec_e = P('e')
    spec_b = P('b')
    spec_qkv = P(None, 'e', ('b', 'x', 'c'))
    spec_qkv_bias = P(None, 'b', None)
    spec_rows_b = P('b', ('e', 'x', 'c'))
    spec_rows_e = P('e', ('b', 'x', 'c'))
    all_specs = (spec_act, spec_act, spec_e, spec_e, spec_qkv, spec_qkv_bias, spec_rows_b,
                 spec_e, spec_e, spec_e, spec_rows_e, spec_b, spec_rows_b, spec_e)

    def local_step(x_loc, dy_loc, ln1_gain, ln1_shift, w_qkv, b_qkv, w_out, b_out, ln2_gain, ln2_shift, w_up, b_up, w_down, b_down):
        seq, cols = x_loc.shape[1], x_loc.shape[2]
        hid = cols * ne
        heads, hd = b_qkv.shape[1] * nb, b_qkv.shape[2]
        ffn = b_up.shape[0] * nb
        hl = hid // nb
        ix = {ax: lax.axis_index(ax) for ax in ('e', 'b', 'x', 'c')}

        ev = jnp.stack([ln1_gain, ln1_shift, b_out, ln2_gain, ln2_shift, b_down])
        bv = jnp.concatenate([b_qkv.reshape(-1), b_up]).reshape(-1, 128)
        wu = lax.all_gather(w_up, AXES).reshape((ne, 8) + w_up.shape)
        wd = lax.all_gather(w_down.T, AXES).reshape((ne, 2, 4) + w_down.T.shape)
        wq, wo, x, ev, bv = gather_all(ne, w_qkv, w_out.T, x_loc, ev, bv)
        dy_loc, x = lax.optimization_barrier((dy_loc, x))
        dy = swap_e(dy_loc).transpose(1, 0, 2).reshape(seq, hid)
        x = x.astype(F32)
        ev = ev.transpose(1, 0, 2).reshape(6, hid)
        ln1_g, ln1_s, bo, ln2_g, ln2_s, bd = [ev[i] for i in range(6)]
        bv = bv.reshape(nb, -1)
        bq = bv[:, :3 * hl].reshape(nb, 3, hl).transpose(1, 0, 2).reshape(3, hid)
        bu = bv[:, 3 * hl:].reshape(ffn)

        h1, n1, i1 = norm_forward(x, ln1_g, ln1_s)
        qkv = qkv_matmul(h1, wq, bq)
        ctx = attend(qkv, hd)
        x1 = (x + ein('sk,nk->sn', ctx, wo) + bo).astype(BF16)
        h2, n2, i2 = norm_forward(x1.astype(F32), ln2_g, ln2_s)
        pre, m = up_matmul(h2, wu, bu)
        g_wd_blocks = grad_rows(dy, m, ne)
        g_wd = scatter(g_wd_blocks)
        y = down_matmul(m, wd, x1, bd)
        y_loc = swap_e(y)

        dyf = dy.astype(F32)
        g_bd = jnp.sum(dyf, axis=0)
        d_pre, g_bu = dact_matmul(dy, wd, pre, g_wd_blocks, y)
        g_bu = g_bu[0]
        g_wu_blocks = grad_cols(h2, d_pre, ne)
        d_h2 = dh_matmul(d_pre, wu, g_wu_blocks)
        d_n2, g_g2, g_s2 = norm_backward(d_h2.astype(F32), n2, i2, ln2_g)
        d_x1 = (dyf + d_n2).astype(BF16)
        d_x1f = d_x1.astype(F32)
        g_bo = jnp.sum(d_x1f, axis=0)
        g_wo = grad_rows(d_x1, ctx, ne)
        d_ctx = ein('sn,nk->sk', d_x1, wo).astype(BF16)
        *d_qkv, g_bq = attend_back(qkv, d_ctx, hd)
        g_bq = g_bq.reshape(-1)
        g_wq = grad_qkv(h1, d_qkv, ne)
        d_h1 = dh1_matmul(d_qkv, wq, y_loc)
        d_n1, g_g1, g_s1 = norm_backward(d_h1.astype(F32), n1, i1, ln1_g)
        g_wd, g_wq, g_wo = lax.optimization_barrier((g_wd, g_wq, g_wo))
        g_wd = scatter_e(g_wd)
        vec = jnp.concatenate([g_bo, g_g2, g_s2, g_bd, g_bq, g_bu, g_g1, g_s1]).reshape(-1, 128)
        g_wu, g_wq, g_wo, gx_loc, vec = finish(ne, g_wu_blocks, g_wq, g_wo, (d_x1f + d_n1).astype(BF16), vec)
        vec = vec.reshape(-1)
        early, late = vec[:7 * hid + ffn], vec[7 * hid + ffn:]

        cut_e = lambda v: lax.dynamic_slice_in_dim(v, ix['e'] * cols, cols)
        r_bo, r_g2, r_s2, r_bd = [cut_e(early[i * hid:(i + 1) * hid]) for i in range(4)]
        r_bq = lax.dynamic_slice_in_dim(early[4 * hid:7 * hid].reshape(3, heads, hd), ix['b'] * (heads // nb), heads // nb, axis=1)
        r_bu = lax.dynamic_slice_in_dim(early[7 * hid:], ix['b'] * (ffn // nb), ffn // nb)
        r_g1, r_s1 = cut_e(late[:hid]), cut_e(late[hid:])
        return (y_loc, gx_loc, r_g1, r_s1, g_wq, r_bq, g_wo.T, r_bo,
                r_g2, r_s2, g_wu, r_bu, g_wd.T, r_bd)

    return jax.shard_map(local_step, mesh=fine, in_specs=all_specs, out_specs=all_specs, check_vma=False)
```

```python
import functools

import jax
import jax.numpy as jnp
from jax import lax
from jax.experimental import pallas as pl
from jax.experimental.pallas import tpu as pltpu
from jax.sharding import Mesh, PartitionSpec as P

LN_EPS = 1e-5
F32 = jnp.float32
BF16 = jnp.bfloat16
AXES = ('e', 'b', 'x', 'c')
HALVES = range(2)
TN = (((0,), (0,)), ((), ()))
NT = (((1,), (1,)), ((), ()))
NN = (((1,), (0,)), ((), ()))


def ein(form, *ops):
    return jnp.einsum(form, *ops, preferred_element_type=F32)


def norm_forward(x_wide, ln_gain, ln_shift):
    row_mean = jnp.mean(x_wide, axis=-1, keepdims=True)
    centered = x_wide - row_mean
    variance = jnp.mean(centered * centered, axis=-1, keepdims=True)
    inv_std = lax.rsqrt(variance + LN_EPS)
    normed = centered * inv_std
    return (normed * ln_gain + ln_shift).astype(BF16), normed, inv_std


def norm_backward(d_wide, normed, inv_std, ln_gain):
    d_normed = d_wide * ln_gain
    mean_d = jnp.mean(d_normed, axis=-1, keepdims=True)
    mean_dn = jnp.mean(d_normed * normed, axis=-1, keepdims=True)
    d_in = inv_std * (d_normed - mean_d - normed * mean_dn)
    return d_in, jnp.sum(d_wide * normed, axis=0), jnp.sum(d_wide, axis=0)


TQ = 256


def low_lanes(shape, hd):
    return lax.broadcasted_iota(jnp.int32, shape, 1) < hd


def attend_body(hd, q, k, v, ctx):
    seq, lanes = q.shape
    for t in range(seq // TQ):
        end = (t + 1) * TQ
        qt, kt, vt = q[t * TQ:end], k[:end], v[:end]
        low = low_lanes(qt.shape, hd)
        zero = jnp.zeros_like(qt)
        keep = lax.broadcasted_iota(jnp.int32, (TQ, end), 0) + t * TQ >= lax.broadcasted_iota(jnp.int32, (TQ, end), 1)
        outs = []
        for head in HALVES:
            qh = jnp.where(low, qt, zero) if head == 0 else jnp.where(low, zero, qt)
            s = jnp.where(keep, dot(qh, kt, NT) * (hd ** -0.5), -1e30)
            s = jnp.exp(s - jnp.max(s, axis=1, keepdims=True))
            p = (s * (1.0 / jnp.sum(s, axis=1, keepdims=True))).astype(BF16)
            outs.append(dot(p, vt, NN))
        ctx[t * TQ:end] = jnp.where(low, outs[0], outs[1]).astype(BF16)


def attend(qkv, hd):
    seq, hid = qkv.shape[0], qkv.shape[1] // 3
    lanes = 2 * hd
    n = hid // lanes
    return tiled_call(functools.partial(attend_body, hd), 'attend', (n,),
                      [cols_of(seq, lanes, g * n) for g in range(3)], cols_of(seq, lanes), jax.ShapeDtypeStruct((seq, hid), BF16),
                      4 * seq * seq * hid, qkv, qkv, qkv)


def down_sum(t):
    return jnp.sum(t, axis=0, keepdims=True)


def down_max(t):
    return jnp.max(t, axis=0, keepdims=True)


def attend_back_body(hd, q, k, v, dctx, dq, dk, dv, sums):
    seq, lanes = q.shape
    tq = seq
    scale = hd ** -0.5
    acc_k = acc_v = None
    for t in range(seq // tq):
        end = (t + 1) * tq
        qt, dt, kt, vt = q[t * tq:end], dctx[t * tq:end], k[:end], v[:end]
        low = low_lanes(qt.shape, hd)
        zero = jnp.zeros_like(qt)
        keep = lax.broadcasted_iota(jnp.int32, (end, tq), 1) + t * tq >= lax.broadcasted_iota(jnp.int32, (end, tq), 0)
        parts = []
        for head in HALVES:
            qh = jnp.where(low, qt, zero) if head == 0 else jnp.where(low, zero, qt)
            dh = jnp.where(low, dt, zero) if head == 0 else jnp.where(low, zero, dt)
            s = jnp.where(keep, dot(kt, qh, NT) * scale, -1e30)
            s = jnp.exp(s - down_max(s))
            p = s * (1.0 / down_sum(s))
            dp = dot(vt, dh, NT).astype(BF16).astype(F32)
            ds = p * (dp - down_sum(dp * p)) * scale
            ds = ds.astype(BF16)
            parts.append((dot(ds, kt, TN),
                          dot(ds, qt, NN), dot(p.astype(BF16), dt, NN)))
        (q0, k0, v0), (q1, k1, v1) = parts
        dq[t * tq:end] = jnp.where(low, q0, q1).astype(BF16)
        low_k = low_lanes((end, lanes), hd)
        pk, pv = jnp.where(low_k, k0, k1), jnp.where(low_k, v0, v1)
        if acc_k is None:
            acc_k, acc_v = pk, pv
        else:
            done = acc_k.shape[0]
            acc_k = jnp.concatenate([acc_k + pk[:done], pk[done:]], axis=0)
            acc_v = jnp.concatenate([acc_v + pv[:done], pv[done:]], axis=0)
    dk[...] = acc_k.astype(BF16)
    dv[...] = acc_v.astype(BF16)
    for g, d in enumerate((dq, dk, dv)):
        sums[g:g + 1] = down_sum(d[...].astype(F32))


def attend_back(qkv, d_ctx, hd):
    seq, hid = d_ctx.shape
    lanes = 2 * hd
    n = hid // lanes
    col = cols_of(seq, lanes)
    o = jax.ShapeDtypeStruct((seq, hid), BF16)
    return tiled_call(functools.partial(attend_back_body, hd), 'attend_back', (n,),
                      [cols_of(seq, lanes, g * n) for g in range(3)] + [col],
                      [col, col, col, cols_of(3, lanes)], [o, o, o, jax.ShapeDtypeStruct((3, hid), F32)],
                      10 * seq * seq * hid, qkv, qkv, qkv, d_ctx)


def qkv_body(h, w, bias, out):
    out[...] = (dot(h[...], w[0], NN) + bias[...]).astype(BF16)


def qkv_matmul(h, wq, bias):
    seq = h.shape[0]
    groups, hid, n = wq.shape
    per = 2
    tile = n // per
    return tiled_call(qkv_body, 'qkv', (groups, per),
                      [whole(h), pl.BlockSpec((1, hid, tile), lambda g, j: (g, 0, j)), pl.BlockSpec((1, tile), lambda g, j: (0, g * per + j))],
                      pl.BlockSpec((seq, tile), lambda g, j: (0, g * per + j)), jax.ShapeDtypeStruct((seq, groups * n), BF16),
                      2 * seq * groups * n * hid, h, wq, bias.reshape(1, groups * n))


def dh1_body(d0, d1, d2, w, dep, dh):
    dh[...] = sum(dot(d[...], w[g], NT) for g, d in enumerate((d0, d1, d2))).astype(BF16)


def dh1_matmul(ds, wq, dep):
    seq, n = ds[0].shape
    groups, hid, _ = wq.shape
    tile = hid // 4
    return tiled_call(dh1_body, 'dh1', (4,),
                      [whole(d) for d in ds] + [pl.BlockSpec((groups, tile, n), lambda j: (0, j, 0)), pl.BlockSpec(memory_space=pl.ANY)],
                      cols_of(seq, tile), jax.ShapeDtypeStruct((seq, hid), BF16),
                      2 * seq * groups * n * hid, *ds, wq, dep)


def gelu_tanh(pre_act):
    return jax.nn.gelu(pre_act, approximate=True)


def scatter(g):
    return lax.psum_scatter(g, AXES[1:])


def swap_e(t):
    return lax.all_to_all(t, 'e', split_axis=0, concat_axis=0, tiled=True)


def scatter_e(g):
    return lax.psum_scatter(g, 'e')


def matmul_t(left_t, right):
    return dot(left_t, right, NN).astype(BF16)


def grad_cols_body(lt, r, o):
    o[...] = matmul_t(lt[...], r[...]).reshape(o.shape)


def grad_cols(left, right, ne):
    seq, rows = left.shape
    width = right.shape[1] // 8
    return tiled_call(grad_cols_body, 'grad_cols', (8,), [whole(left.T), cols_of(seq, width)],
                      pl.BlockSpec((1, ne, rows // ne, width), lambda j: (j, 0, 0, 0)),
                      jax.ShapeDtypeStruct((8, ne, rows // ne, width), BF16), 16 * seq * rows * width, left.T, right)


def grad_qkv_body(lt, r0, r1, r2, o):
    width = o.shape[-1]
    for g, r in enumerate((r0, r1, r2)):
        full = matmul_t(lt[...], r[...]).reshape(o.shape[1], o.shape[3], 2 * width)
        o[0, :, g] = full[:, :, :width]
        o[1, :, g] = full[:, :, width:]


def grad_qkv(left, rights, ne):
    seq, rows = left.shape
    width = rights[0].shape[1] // 8
    return tiled_call(grad_qkv_body, 'grad_qkv', (4,), [whole(left.T)] + [cols_of(seq, 2 * width)] * 3,
                      pl.BlockSpec((2, ne, 3, rows // ne, width), lambda j: (j, 0, 0, 0, 0)),
                      jax.ShapeDtypeStruct((8, ne, 3, rows // ne, width), BF16), 48 * seq * rows * width, left.T, *rights)


def grad_rows_body(lt, r, o):
    full = matmul_t(lt[...], r[...]).reshape(o.shape[2], o.shape[1], o.shape[3], o.shape[4])
    for e in range(o.shape[2]):
        o[0, :, e] = full[e]


def grad_rows(left, right, ne):
    seq, rows = left.shape
    width = right.shape[1] // 2
    tile = min(width, 512)
    per = width // tile
    rr = rows // (4 * ne)
    out = tiled_call(grad_rows_body, 'grad_rows', (2 * per,), [whole(left.T), cols_of(seq, tile)],
                     pl.BlockSpec((1, 4, ne, rr, tile), lambda j: (j // per, 0, 0, 0, j % per)),
                     jax.ShapeDtypeStruct((2, 4, ne, rr, width), BF16), 4 * seq * rows * width, left.T, right)
    return out.reshape(8, ne, rr, width)


def region(kind, ref, e, h, b, x, c, width):
    if kind == 'qkv':
        return ref.at[:, e, h, :, pl.ds(pl.multiple_of((b * 4 + x * 2 + c) * width, width), width)]
    return ref.at[e, x, c, h, :, pl.ds(pl.multiple_of(b * width, width), width)]


KINDS = ('qkv', 'row')
ALLS = slice(None)


def gather_kernel(ne, *refs):
    (wq, wo, xin, evin, bvin, gq, go, xo, evo, bvo, ssem, rsem, lsem) = refs
    e, b, x, c = (lax.axis_index(ax) for ax in AXES)
    ob, ox, oc = (1 - t for t in (b, x, c))
    px, pb, pc = {'x': ox}, {'b': ob}, {'c': oc}
    blocks, fulls = (wq, wo), (gq, go)
    nw = len(blocks)
    widths = tuple(w.shape[-1] for w in blocks)
    mesh_id = pl.DeviceIdType.MESH
    peers = [{'e': lax.rem(e + k, ne)} for k in range(1, ne)] + [px, pb, pc]
    barrier = pltpu.get_barrier_semaphore()
    for peer in peers:
        pl.semaphore_signal(barrier, inc=1, device_id=peer, device_id_type=mesh_id)
    pl.semaphore_wait(barrier, len(peers))

    sent = []

    def send(src, dst, peer):
        n = len(sent)
        copy = pltpu.make_async_remote_copy(src_ref=src, dst_ref=dst, send_sem=ssem.at[n], recv_sem=rsem.at[n],
                                            device_id=peer, device_id_type=mesh_id)
        copy.start()
        sent.append(copy)
        return copy

    kept = []

    def keep(src, dst):
        copy = pltpu.make_async_copy(src, dst, lsem.at[len(kept)])
        copy.start()
        kept.append(copy)
        return copy

    def to_z(src_of, dst):
        return [send(src_of(lax.rem(e + k, ne)), dst, {'e': lax.rem(e + k, ne)}) for k in range(1, ne)]

    def at(w, ee, h, bb, xx):
        return region(KINDS[w], fulls[w], ee, h, bb, xx, c, widths[w])

    def block(w):
        return blocks[w].at[...]

    cols = xin.shape[2]
    mine = pl.ds(pl.multiple_of(e * cols, cols), cols)
    z, own = {}, {}
    for w in range(nw):
        own[w] = keep(block(w), at(w, e, ALLS, b, x))
    keep(evin.at[...], evo.at[e])
    keep(bvin.at[...], bvo.at[b])
    keep(xin.at[e], xo.at[:, mine])
    waits = []
    z[0] = to_z(lambda t: block(0), at(0, e, ALLS, b, x))
    waits += to_z(lambda t: evin.at[...], evo.at[e])
    waits.append(send(bvin.at[...], bvo.at[b], pb))
    waits += to_z(lambda t: xin.at[t], xo.at[:, mine])
    for w in range(1, nw):
        z[w] = to_z(lambda t, w=w: block(w), at(w, e, ALLS, b, x))

    first, second = {}, {}

    def move(w, h, bb, xx, peer):
        r = at(w, ALLS, h, bb, xx)
        return send(r, r, peer)

    def after_z(w):
        own[w].wait()
        for copy in z[w]:
            copy.wait_recv()
        first[w] = [move(w, 0, b, x, px), move(w, 1, b, x, pb)]
        second[w] = [move(w, 0, b, x, pb), move(w, 1, b, x, px)]
        waits.append(move(w, ALLS, b, x, pc))

    def after_first(w):
        first[w][0].wait_recv()
        second[w].append(move(w, 0, b, ox, pb))
        first[w][1].wait_recv()
        second[w].append(move(w, 1, ob, x, px))
        waits.append(move(w, 0, b, ox, pc))
        waits.append(move(w, 1, ob, x, pc))

    def after_second(w):
        for n, (h, bb, xx) in enumerate(((0, ob, x), (1, b, ox), (0, ob, ox), (1, ob, ox))):
            second[w][n].wait_recv()
            waits.append(move(w, h, bb, xx, pc))

    for w in range(nw + 2):
        if w < nw:
            after_z(w)
        if 1 <= w < nw + 1:
            after_first(w - 1)
        if w >= 2:
            after_second(w - 2)
    for copy in waits:
        copy.wait_recv()
    for copy in sent:
        copy.wait_send()
    for copy in kept[nw:]:
        copy.wait()


N_SENDS = 2 * 16 + 2 * 3 + 1


def gather_all(ne, w_qkv, w_out_t, x_loc, ev, bv):
    g3, kq, nq = w_qkv.shape
    ko, no = w_out_t.shape
    seq, cols = x_loc.shape[1], x_loc.shape[2]
    s = lambda shape, dt=BF16: jax.ShapeDtypeStruct(shape, dt)
    outs = [s((g3, ne, 2, kq // 2, 8 * nq)), s((ne, 2, 2, 2, ko // 2, 2 * no)), s((seq, ne * cols)),
            s((ne,) + ev.shape, F32), s((2,) + bv.shape, F32)]
    vm = pl.BlockSpec(memory_space=pltpu.VMEM)
    hbm = pl.BlockSpec(memory_space=pl.ANY)
    gq, go, x, evo, bvo = pl.pallas_call(
        functools.partial(gather_kernel, ne),
        out_shape=outs,
        in_specs=[vm] * 5,
        out_specs=[hbm] * 5,
        scratch_shapes=[pltpu.SemaphoreType.DMA((N_SENDS,)), pltpu.SemaphoreType.DMA((N_SENDS,)), pltpu.SemaphoreType.DMA((5,))],
        compiler_params=pltpu.CompilerParams(collective_id=0, has_side_effects=True),
        name='gather_all',
    )(w_qkv.reshape(g3, 2, kq // 2, nq), w_out_t.reshape(2, ko // 2, no), x_loc, ev, bv)
    return gq.reshape(g3, ne * kq, 8 * nq), go.reshape(ne * 4 * ko, 2 * no), x, evo, bvo


def dot(left, right, dims):
    return lax.dot_general(left, right, dims, preferred_element_type=F32)


def tiled_call(body, name, grid, in_specs, out_specs, out_shape, flops, *args):
    return pl.pallas_call(body, grid=grid, in_specs=in_specs, out_specs=out_specs, out_shape=out_shape, name=name,
                          compiler_params=pltpu.CompilerParams(vmem_limit_bytes=56 * 1024 * 1024),
                          cost_estimate=pl.CostEstimate(flops=flops, bytes_accessed=flops // 256, transcendentals=0))(*args)


def whole(t):
    return pl.BlockSpec(t.shape, lambda *i: (0,) * t.ndim)


def cols_of(rows, width, start=0):
    return pl.BlockSpec((rows, width), lambda j: (0, start + j))


def up_body(h, w, bias, pre, act):
    p = dot(h[...], w[...].reshape(h.shape[1], -1), NN) + bias[...]
    pre[...] = p
    act[...] = gelu_tanh(p).astype(BF16)


def up_matmul(h, wu, bias):
    seq = h.shape[0]
    ne, nj, rows, width = wu.shape
    ffn = nj * width
    out = cols_of(seq, width)
    return tiled_call(up_body, 'up', (nj,),
                      [whole(h), pl.BlockSpec((ne, 1, rows, width), lambda j: (0, j, 0, 0)), cols_of(1, width)],
                      [out, out], [jax.ShapeDtypeStruct((seq, ffn), F32), jax.ShapeDtypeStruct((seq, ffn), BF16)],
                      2 * seq * ffn * h.shape[1], h, wu, bias.reshape(1, ffn))


def down_body(m, w, res, bias, y):
    half = w.shape[-1]
    p = res[...].astype(F32) + bias[...]
    for b in range(w.shape[1]):
        p += dot(m[:, b * half:(b + 1) * half], w[0, b].reshape(-1, half), NT)
    y[0] = p.astype(BF16)


def down_matmul(m, wd, res, bias):
    seq, ffn = m.shape
    ne, nb, xc, rows, half = wd.shape
    hid = ne * xc * rows
    tile = cols_of(seq, xc * rows)
    return tiled_call(down_body, 'down', (ne,),
                      [whole(m), pl.BlockSpec((1, nb, xc, rows, half), lambda e: (e, 0, 0, 0, 0)), tile,
                       cols_of(1, xc * rows)],
                      pl.BlockSpec((1, seq, xc * rows), lambda e: (e, 0, 0)), jax.ShapeDtypeStruct((ne, seq, xc * rows), BF16),
                      2 * seq * ffn * hid, m, wd, res, bias.reshape(1, hid))


GELU_A, GELU_B = 0.7978845608028654, 0.044715


def dact_body(dy, w, pre, dep0, dep1, dpre, bsum):
    width = w.shape[-1]
    d = dot(dy[...], w[...].reshape(dy.shape[1], width), NN).astype(BF16).astype(F32)
    p = pre[...]
    sq = p * p
    t = jnp.tanh(GELU_A * (p + GELU_B * (sq * p)))
    slope = 0.5 * (1.0 + t) + 0.5 * p * (1.0 - t * t) * (GELU_A * (1.0 + 3.0 * GELU_B * sq))
    d = d * slope
    bsum[...] = down_sum(d)
    dpre[...] = d.astype(BF16)


def dact_matmul(dy, wd, pre, *deps):
    seq, hid = dy.shape
    ne, nb, xc, rows, half = wd.shape
    ffn, tile = nb * half, min(half, 512)
    per = half // tile
    col = lambda b, n: (0, b * per + n)
    return tiled_call(dact_body, 'dact', (nb, per),
                      [whole(dy), pl.BlockSpec((ne, 1, xc, rows, tile), lambda b, n: (0, b, 0, 0, n)), pl.BlockSpec((seq, tile), col)]
                      + [pl.BlockSpec(memory_space=pl.ANY)] * 2,
                      [pl.BlockSpec((seq, tile), col), pl.BlockSpec((1, tile), col)],
                      [jax.ShapeDtypeStruct((seq, ffn), BF16), jax.ShapeDtypeStruct((1, ffn), F32)],
                      2 * seq * ffn * hid, dy, wd, pre, *deps)


def dh_body(dpre, w, dep, dh):
    width = w.shape[-1]
    dh[...] = sum(dot(dpre[:, j * width:(j + 1) * width], w[0, j], NT) for j in range(w.shape[1])).astype(BF16)


def dh_matmul(dpre, wu, dep):
    seq, ffn = dpre.shape
    ne, nj, rows, width = wu.shape
    return tiled_call(dh_body, 'dh2', (ne,),
                      [whole(dpre), pl.BlockSpec((1, nj, rows, width), lambda e: (e, 0, 0, 0)), pl.BlockSpec(memory_space=pl.ANY)],
                      cols_of(seq, rows), jax.ShapeDtypeStruct((seq, ne * rows), BF16),
                      2 * seq * ffn * ne * rows, dpre, wu, dep)


def finish_kernel(ne, kinds, *refs):
    nm, nc = 3, len(kinds)
    mats, (xin, vin) = refs[:nm], refs[nm:nm + 2]
    outs, (xo, vout) = refs[nm + 2:2 * nm + 2], refs[2 * nm + 2:2 * nm + 4]
    scratch = refs[2 * nm + 4:]
    rc, r1, s1, r2, s2, rz, s3 = (scratch[n * nc:(n + 1) * nc] for n in range(7))
    near, (vr, vs, ve, ssem, rsem, lsem) = scratch[7 * nc:7 * nc + nm], scratch[7 * nc + nm:]
    e, b, x, c = (lax.axis_index(ax) for ax in AXES)
    ob, ox, oc = (1 - t for t in (b, x, c))
    mesh_id = pl.DeviceIdType.MESH
    px, pb, pc = {'x': ox}, {'b': ob}, {'c': oc}
    zs = [lax.rem(e + k, ne) for k in range(1, ne)]
    loads = [pltpu.make_async_copy(mats[m].at[:, :, c], near[m], lsem.at[1 + m]) for m in range(nm)]
    for copy in loads:
        copy.start()
    barrier = pltpu.get_barrier_semaphore()
    peers = [{'e': t} for t in zs] + [px, pb, pc]
    for peer in peers:
        pl.semaphore_signal(barrier, inc=1, device_id=peer, device_id_type=mesh_id)
    pl.semaphore_wait(barrier, len(peers))
    sent = []

    def send(src, dst, peer):
        n = len(sent)
        copy = pltpu.make_async_remote_copy(src_ref=src, dst_ref=dst, send_sem=ssem.at[n], recv_sem=rsem.at[n],
                                            device_id=peer, device_id_type=mesh_id)
        copy.start()
        sent.append(copy)
        return copy

    def piece(n, bb, xx, cc):
        mat, part = kinds[n]
        ref = mats[mat]
        return ref.at[bb, xx, cc] if part is None else ref.at[bb, xx, cc, :, part]

    def own(n, bb, xx, ee, h):
        mat, part = kinds[n]
        ref = near[mat]
        if mat == 1:
            return ref[bb, xx, ee, :, h]
        return ref[bb, xx, ee, h] if part is None else ref[bb, xx, ee, part, h]

    def base(n, bb, xx, ee, h):
        got = rc[n][bb, xx, ee, :, h] if kinds[n][0] == 1 else rc[n][bb, xx, ee, h]
        return own(n, bb, xx, ee, h).astype(F32) + got.astype(F32)

    def over_e(f):
        lax.fori_loop(0, ne, lambda ee, _: (f(ee), 0)[1], 0)

    pairs = ((ob, ox), (b, ox), (ob, x), (b, x))
    core = [[send(piece(n, bb, xx, oc), rc[n].at[bb, xx], pc) for bb, xx in pairs] for n in range(nc)]
    vec = [send(vin, vr.at[0], pc)]
    cols = xin.shape[1] // ne
    col = lambda t: pl.ds(pl.multiple_of(t * cols, cols), cols)
    keep = pltpu.make_async_copy(xin.at[:, col(e)], xo.at[e], lsem.at[0])
    keep.start()
    acts = [send(xin.at[:, col(t)], xo.at[e], {'e': t}) for t in zs]
    one, two, three = {}, {}, {}

    def stage_one(n):
        if not n or kinds[n - 1][0] != kinds[n][0]:
            loads[kinds[n][0]].wait()
        for copy in core[n]:
            copy.wait_recv()
        for i in HALVES:
            for h in HALVES:
                bb, xx = (i, ox) if h == 0 else (ob, i)

                def add(ee):
                    s1[n][h, i, ee] = base(n, bb, xx, ee, h).astype(BF16)

                over_e(add)
                one[n, h, i] = send(s1[n].at[h, i], r1[n].at[h, i], px if h == 0 else pb)

    def stage_two(n):
        for i in HALVES:
            for h in HALVES:
                one[n, h, i].wait_recv()
        for h in HALVES:
            bb, xx, i = (ob, x, ob) if h == 0 else (b, ox, ox)

            def add(ee):
                s2[n][h, ee] = (base(n, bb, xx, ee, h) + r1[n][h, i, ee].astype(F32)).astype(BF16)

            over_e(add)
            two[n, h] = send(s2[n].at[h], r2[n].at[h], pb if h == 0 else px)

    def mine(n, h, ee):
        return base(n, b, x, ee, h) + r1[n][h, b if h == 0 else x, ee].astype(F32) + r2[n][h, ee].astype(F32)

    def stage_three(n):
        for h in HALVES:
            two[n, h].wait_recv()
        for k, t in enumerate(zs):
            for h in HALVES:
                s3[n][k, h] = mine(n, h, t).astype(BF16)
            three[n, k] = send(s3[n].at[k], rz[n].at[k], {'e': t})

    def stage_four(n):
        for k in range(ne - 1):
            three[n, k].wait_recv()
        mat, part = kinds[n]
        for h in HALVES:
            acc = mine(n, h, e)
            for k in range(ne - 1):
                acc = acc + rz[n][k, h].astype(F32)
            if mat == 1:
                outs[mat][:, h] = acc.astype(BF16)
            elif part is None:
                outs[mat][h] = acc.astype(BF16)
            else:
                outs[mat][part, h] = acc.astype(BF16)

    def vec_step(step):
        vec[-1].wait_recv()
        if step < 2:
            vs[step] = (vin[...] if step == 0 else vs[0]) + vr[step]
            vec.append(send(vs.at[step], vr.at[step + 1], px if step == 0 else pb))
        else:
            ve[e] = vs[1] + vr[2]
            vec.extend(send(ve.at[e], ve.at[e], {'e': t}) for t in zs)

    for t in range(nc + 3):
        if t < nc:
            stage_one(t)
        if 1 <= t < nc + 1:
            stage_two(t - 1)
        if 2 <= t < nc + 2:
            stage_three(t - 2)
        if t >= 3:
            stage_four(t - 3)
        if 1 <= t <= 3:
            vec_step(t - 1)
    for copy in vec[3:]:
        copy.wait_recv()
    acc = ve[0]
    for t in range(1, ne):
        acc = acc + ve[t]
    vout[...] = acc
    for copy in acts:
        copy.wait_recv()
    for copy in sent:
        copy.wait_send()
    keep.wait()


def finish(ne, g_wu, g_wq, g_wo, gx, vec):
    _, _, ku, nu = g_wu.shape
    _, _, g3, kq, nq = g_wq.shape
    _, _, ko, no = g_wo.shape
    seq, hid = gx.shape
    parts = 2
    kinds = tuple((0, p) for p in range(parts)) + ((1, None), (2, None))
    u, q, o = (ku // parts // 2, nu), (g3, kq // 2, nq), (ko // 2, no)
    blocks = [u] * parts + [q, o]
    full = [(2,) + u] * parts + [(g3, 2) + q[1:], (2,) + o]
    bf = lambda *shape: pltpu.VMEM(shape, BF16)
    s = lambda *shape: jax.ShapeDtypeStruct(shape, BF16)
    vm = pl.BlockSpec(memory_space=pltpu.VMEM)
    hbm = pl.BlockSpec(memory_space=pl.ANY)
    n = 13 * len(kinds) + 3 + 3 + ne - 1
    f32 = lambda *lead: pltpu.VMEM(lead + vec.shape, F32)
    scratch = ([bf(2, 2, ne, *t) for t in full] + [bf(2, 2, ne, *t) for t in blocks] * 2 + [bf(2, ne, *t) for t in blocks] * 2
               + [bf(ne - 1, 2, *t) for t in blocks] * 2)
    near = [bf(2, 2, ne, parts, 2, *u), bf(2, 2, ne, g3, 2, *q[1:]), bf(2, 2, ne, 2, *o)]
    ru, rq, ro, xo, vo = pl.pallas_call(
        functools.partial(finish_kernel, ne, kinds),
        out_shape=[s(parts, 2, *u), s(g3, 2, *q[1:]), s(2, *o), s(ne, seq, hid // ne), jax.ShapeDtypeStruct(vec.shape, F32)],
        in_specs=[hbm] * 3 + [vm] * 2,
        out_specs=[vm, vm, vm, hbm, vm],
        scratch_shapes=scratch + near + [f32(3), f32(2), f32(ne), pltpu.SemaphoreType.DMA((n,)), pltpu.SemaphoreType.DMA((n,)),
                                  pltpu.SemaphoreType.DMA((4,))],
        compiler_params=pltpu.CompilerParams(collective_id=1, has_side_effects=True, vmem_limit_bytes=60 * 1024 * 1024),
        name='finish',
    )(g_wu.reshape((2, 2, 2, ne, parts, 2) + u), g_wq.reshape((2, 2, 2, ne, g3, 2) + q[1:]), g_wo.reshape((2, 2, 2, ne, 2) + o), gx, vec)
    return ru.reshape(ku, nu), rq.reshape(g3, kq, nq), ro.reshape(ko, no), xo, vo


def solution(mesh):
    ne, nb = mesh.shape['e'], mesh.shape['b']
    fine = Mesh(mesh.devices.reshape(ne, nb, 2, 2), ('e', 'b', 'x', 'c'))
    spec_act = P(('x', 'c', 'b'), None, 'e')
    spec_e = P('e')
    spec_b = P('b')
    spec_qkv = P(None, 'e', ('b', 'x', 'c'))
    spec_qkv_bias = P(None, 'b', None)
    spec_rows_b = P('b', ('e', 'x', 'c'))
    spec_rows_e = P('e', ('b', 'x', 'c'))
    all_specs = (spec_act, spec_act, spec_e, spec_e, spec_qkv, spec_qkv_bias, spec_rows_b,
                 spec_e, spec_e, spec_e, spec_rows_e, spec_b, spec_rows_b, spec_e)

    def local_step(x_loc, dy_loc, ln1_gain, ln1_shift, w_qkv, b_qkv, w_out, b_out, ln2_gain, ln2_shift, w_up, b_up, w_down, b_down):
        seq, cols = x_loc.shape[1], x_loc.shape[2]
        hid = cols * ne
        heads, hd = b_qkv.shape[1] * nb, b_qkv.shape[2]
        ffn = b_up.shape[0] * nb
        hl = hid // nb
        ix = {ax: lax.axis_index(ax) for ax in ('e', 'b', 'x', 'c')}

        ev = jnp.stack([ln1_gain, ln1_shift, b_out, ln2_gain, ln2_shift, b_down])
        bv = jnp.concatenate([b_qkv.reshape(-1), b_up]).reshape(-1, 128)
        wu = lax.all_gather(w_up, AXES).reshape((ne, 8) + w_up.shape)
        wd = lax.all_gather(w_down.T, AXES).reshape((ne, 2, 4) + w_down.T.shape)
        wq, wo, x, ev, bv = gather_all(ne, w_qkv, w_out.T, x_loc, ev, bv)
        dy_loc, x = lax.optimization_barrier((dy_loc, x))
        dy = swap_e(dy_loc).transpose(1, 0, 2).reshape(seq, hid)
        x = x.astype(F32)
        ev = ev.transpose(1, 0, 2).reshape(6, hid)
        ln1_g, ln1_s, bo, ln2_g, ln2_s, bd = [ev[i] for i in range(6)]
        bv = bv.reshape(nb, -1)
        bq = bv[:, :3 * hl].reshape(nb, 3, hl).transpose(1, 0, 2).reshape(3, hid)
        bu = bv[:, 3 * hl:].reshape(ffn)

        h1, n1, i1 = norm_forward(x, ln1_g, ln1_s)
        qkv = qkv_matmul(h1, wq, bq)
        ctx = attend(qkv, hd)
        x1 = (x + ein('sk,nk->sn', ctx, wo) + bo).astype(BF16)
        h2, n2, i2 = norm_forward(x1.astype(F32), ln2_g, ln2_s)
        pre, m = up_matmul(h2, wu, bu)
        g_wd_blocks = grad_rows(dy, m, ne)
        g_wd = scatter(g_wd_blocks)
        y = down_matmul(m, wd, x1, bd)
        y_loc = swap_e(y)

        dyf = dy.astype(F32)
        g_bd = jnp.sum(dyf, axis=0)
        d_pre, g_bu = dact_matmul(dy, wd, pre, g_wd_blocks, y)
        g_bu = g_bu[0]
        g_wu_blocks = grad_cols(h2, d_pre, ne)
        d_h2 = dh_matmul(d_pre, wu, g_wu_blocks)
        d_n2, g_g2, g_s2 = norm_backward(d_h2.astype(F32), n2, i2, ln2_g)
        d_x1 = (dyf + d_n2).astype(BF16)
        d_x1f = d_x1.astype(F32)
        g_bo = jnp.sum(d_x1f, axis=0)
        g_wo = grad_rows(d_x1, ctx, ne)
        d_ctx = ein('sn,nk->sk', d_x1, wo).astype(BF16)
        *d_qkv, g_bq = attend_back(qkv, d_ctx, hd)
        g_bq = g_bq.reshape(-1)
        g_wq = grad_qkv(h1, d_qkv, ne)
        d_h1 = dh1_matmul(d_qkv, wq, y_loc)
        d_n1, g_g1, g_s1 = norm_backward(d_h1.astype(F32), n1, i1, ln1_g)
        g_wd, g_wq, g_wo = lax.optimization_barrier((g_wd, g_wq, g_wo))
        g_wd = scatter_e(g_wd)
        vec = jnp.concatenate([g_bo, g_g2, g_s2, g_bd, g_bq, g_bu, g_g1, g_s1]).reshape(-1, 128)
        g_wu, g_wq, g_wo, gx_loc, vec = finish(ne, g_wu_blocks, g_wq, g_wo, (d_x1f + d_n1).astype(BF16), vec)
        vec = vec.reshape(-1)
        early, late = vec[:7 * hid + ffn], vec[7 * hid + ffn:]

        cut_e = lambda v: lax.dynamic_slice_in_dim(v, ix['e'] * cols, cols)
        r_bo, r_g2, r_s2, r_bd = [cut_e(early[i * hid:(i + 1) * hid]) for i in range(4)]
        r_bq = lax.dynamic_slice_in_dim(early[4 * hid:7 * hid].reshape(3, heads, hd), ix['b'] * (heads // nb), heads // nb, axis=1)
        r_bu = lax.dynamic_slice_in_dim(early[7 * hid:], ix['b'] * (ffn // nb), ffn // nb)
        r_g1, r_s1 = cut_e(late[:hid]), cut_e(late[hid:])
        return (y_loc, gx_loc, r_g1, r_s1, g_wq, r_bq, g_wo.T, r_bo,
                r_g2, r_s2, g_wu, r_bu, g_wd.T, r_bd)

    return jax.shard_map(local_step, mesh=fine, in_specs=all_specs, out_specs=all_specs, check_vma=False)
```
